128 devices in a mesh: bank: 4 (over y), zero: 32 (over z, x, core).
Axes of the slice: x: 4, y: 4, z: 4, core: 2. Of those that a mesh axis runs over, the one named last changes fastest.
Arguments:
- train_gate: float32 [64, 2048, 1024], P('bank', 'zero'), may hold values from -0.25 to 0.25
- train_up: float32 [64, 2048, 1024], P('bank', 'zero'), may hold values from -0.25 to 0.25
- train_down: float32 [64, 1024, 2048], P('bank', None, 'zero'), may hold values from -0.375 to 0.375
- router_weight: float32 [2048, 64], P('zero', 'bank'), may hold values from -0.125 to 0.125
- router_gain: float32 [2048], P('zero'), may hold values from 0.25 to 1.75
Outputs:
- ready_gate: bfloat16 [64, 2048, 1024], P('bank', None, 'zero')
- ready_up: bfloat16 [64, 2048, 1024], P('bank', None, 'zero')
- ready_down: bfloat16 [64, 1024, 2048], P('bank', 'zero')
- scale_gate: float32 [64, 1024], P('bank', 'zero')
- scale_up: float32 [64, 1024], P('bank', 'zero')
- scale_down: float32 [64, 1024], P('bank', 'zero')
- serve_router: bfloat16 [2048, 64], replicated
The draws below stay inside these ranges and needn't reach their ends.
All inputs are finite; a program needn't handle non-finite values.
Results may differ from the reference program's by a relative error of at most 0.001.
Values may be sent and summed in bfloat16 or wider, within the bound.
A program may use at most 128 MiB of HBM per device.

```python
import jax
import jax.numpy as jnp
from jax import lax

EXPERTS = 64
D_MODEL = 2048
D_EXPERT = 1024


def spiked(result, rng, source, target, blocks, factor):
    owner, partner = [(jnp.arange(result.shape[axis_at]) // (result.shape[axis_at] // blocks)).reshape([-1 if axis == axis_at else 1 for axis in range(result.ndim)]) for axis_at in (source, target)]
    chosen = jax.random.permutation(rng, blocks)[partner]
    strong = (owner == chosen) | (owner == (partner + blocks // 2) % blocks)
    return jnp.where(strong, factor * result, result)


def level_of(rng, shape, shards, least, top_value):
    factor_of, own = 1.0, jax.random.fold_in(rng, 6)
    for axis_at, shards_of in shards:
        heights = jnp.exp(jax.random.uniform(jax.random.fold_in(own, axis_at), (shards_of,), jnp.float32, least / len(shards), top_value / len(shards)))
        factor_of = factor_of * jnp.repeat(heights, shape[axis_at] // shards_of).reshape([-1 if axis == axis_at else 1 for axis in range(len(shape))])
    return factor_of


def scatter_about(own_key, shape, spread, limit, split=(), dtype=jnp.bfloat16):
    array = spread * jax.random.normal(own_key, shape, jnp.float32)
    if split:
        array = array * level_of(own_key, shape, split, -0.22, 0.18)
    return jnp.clip(array, -limit, limit).astype(dtype)


def noise_with(stream_key, extent, scale, reach, split, heavy, kind=jnp.bfloat16):
    drawn = scale * jax.random.normal(stream_key, extent, jnp.float32)
    if split:
        drawn = drawn * level_of(stream_key, extent, split, -0.22, 0.18)
    return jnp.clip(spiked(drawn, jax.random.fold_in(stream_key, 3), *heavy), -reach, reach).astype(kind)


def setup_inputs(seed: int = 0) -> dict:
    streams_of = jax.random.split(jax.random.key(seed), 6)
    return {
        "train_gate": noise_with(streams_of[0], (EXPERTS, D_MODEL, D_EXPERT), D_MODEL ** -0.5, 0.25, ((0, 4), (1, 32)), (1, 2, 32, 2.75), jnp.float32),
        "train_up": noise_with(streams_of[1], (EXPERTS, D_MODEL, D_EXPERT), D_MODEL ** -0.5, 0.25, ((0, 4), (1, 32)), (1, 2, 32, 2.75), jnp.float32),
        "train_down": noise_with(streams_of[2], (EXPERTS, D_EXPERT, D_MODEL), D_EXPERT ** -0.5, 0.375, ((0, 4), (2, 32)), (2, 1, 32, 2.75), jnp.float32),
        "router_weight": scatter_about(streams_of[3], (D_MODEL, EXPERTS), D_MODEL ** -0.5, 0.125, ((0, 32), (1, 4)), jnp.float32),
        "router_gain": jnp.clip(1.0 + 0.15 * jax.random.normal(streams_of[4], (D_MODEL,), jnp.float32), 0.25, 1.75),
    }


def reference(train_gate, train_up, train_down, router_weight, router_gain):
    scale_gate = jnp.sqrt(lax.optimization_barrier(jnp.sum(train_gate * train_gate, axis=1)))
    ready_gate = (train_gate / jnp.expand_dims(scale_gate, 1)).astype(jnp.bfloat16)
    scale_up = jnp.sqrt(lax.optimization_barrier(jnp.sum(train_up * train_up, axis=1)))
    ready_up = (train_up / jnp.expand_dims(scale_up, 1)).astype(jnp.bfloat16)
    scale_down = jnp.sqrt(lax.optimization_barrier(jnp.sum(train_down * train_down, axis=2)))
    ready_down = (train_down / jnp.expand_dims(scale_down, 2)).astype(jnp.bfloat16)
    serve_router = (router_weight * router_gain[:, None]).astype(jnp.bfloat16)
    return (ready_gate, ready_up, ready_down, scale_gate, scale_up, scale_down, serve_router)
```

```python
import jax
import jax.numpy as jnp
from jax import lax
from jax.experimental import pallas as pl
from jax.experimental.pallas import tpu as pltpu
from jax.sharding import PartitionSpec as P

MESH = pl.DeviceIdType.MESH
ZERO = 32
CHUNKS = 6
PAIRS = 24
PER = PAIRS // CHUNKS
ROWS = PER * 32
POWER = 20
UP = 2.0**6.25
ORDER = (
    (0, 1), (3, 0), (2, 3), (1, 1), (3, 3), (0, 2), (1, 0), (3, 1),
    (1, 3), (2, 2), (2, 0), (0, 3), (1, 2), (3, 2), (2, 1),
)
OFFSETS = tuple((z, x, c) for z, x in ORDER for c in (0, 1))


def exchange(
    gate, up, down, weight, gain,
    out, scale, router,
    xin, send, recv, sums, sums_send, sums_recv, table, part_send, part_recv,
    in_sem, send_sem, recv_sem, sums_send_sem, sums_recv_sem,
    part_send_sem, part_recv_sem, row_send_sem, row_recv_sem,
):
    me = lax.axis_index("zero")
    bank = lax.axis_index("bank")
    mz, mx, mc = lax.div(me, 8), lax.rem(lax.div(me, 2), 4), lax.rem(me, 2)

    def peer(offset):
        z, x, c = offset
        return (
            lax.rem(mz + z, 4) * 8 + lax.rem(mx + x, 4) * 2 + lax.rem(mc + c, 2)
        )

    loads = []
    for a, ref in enumerate((gate, up, down)):
        for h in range(2):
            copy = pltpu.make_async_copy(
                ref.at[pl.ds(8 * h, 8)],
                xin.at[pl.ds(16 * a + 8 * h, 8)],
                in_sem.at[2 * a + h],
            )
            copy.start()
            loads.append(copy)

    barrier = pltpu.get_barrier_semaphore()

    def greet(i, _):
        pl.semaphore_signal(
            barrier,
            inc=1,
            device_id={"zero": lax.rem(me + i, ZERO)},
            device_id_type=MESH,
        )
        return 0

    lax.fori_loop(1, ZERO, greet, 0)
    for i in range(1, 4):
        pl.semaphore_signal(
            barrier,
            inc=1,
            device_id={"bank": lax.rem(bank + i, 4)},
            device_id_type=MESH,
        )

    part = (weight[...] * gain[...]).astype(jnp.bfloat16)
    packed = jnp.concatenate([part[0:8], part[8:16]], axis=1)
    part_send[...] = packed
    part_recv[me] = packed

    def add_up(e, _):
        x = xin[e]
        sums[e] = jnp.sum(x * x, axis=0, keepdims=True)
        return 0

    def code_pair(c):
        def go(k, _):
            p = c * PER + k
            for b in range(8):
                columns = slice(128 * b, 128 * b + 128)
                halves = []
                for e in range(2):
                    s = sums[2 * p + e, :, columns]
                    r = jnp.where(s > 0.0, lax.rsqrt(s) * UP, 0.0)
                    halves.append(xin[2 * p + e, :, columns] * r)
                y = jnp.concatenate(halves, axis=0).T
                y2 = y * y
                y4 = y2 * y2
                y8 = y4 * y4
                y20 = y8 * y8 * y4
                u = jnp.where(y < 0.0, -y20, y20).astype(jnp.bfloat16)
                for q in range(4):
                    send[c, 4 * b + q, pl.ds(pl.multiple_of(32 * k, 32), 32), :] = u[
                        32 * q : 32 * q + 32
                    ]
            return 0

        return go

    def send_chunk(c):
        for offset in OFFSETS:
            d = peer(offset)
            pltpu.make_async_remote_copy(
                src_ref=send.at[c, d],
                dst_ref=recv.at[c, me],
                send_sem=send_sem.at[c],
                recv_sem=recv_sem.at[c],
                device_id={"zero": d},
                device_id_type=MESH,
            ).start()
        d = peer((0, 0, 1))
        pltpu.make_async_remote_copy(
            src_ref=send.at[c, d],
            dst_ref=recv.at[c, me],
            send_sem=send_sem.at[c],
            recv_sem=recv_sem.at[c],
            device_id={"zero": d},
            device_id_type=MESH,
        ).start()
        recv[c, me] = send[c, me]

    loads[0].wait()
    lax.fori_loop(0, 8, add_up, 0)
    lax.fori_loop(0, PER, code_pair(0), 0)
    pl.semaphore_wait(barrier, ZERO - 1 + 3)
    send_chunk(0)

    for i in range(1, 6):
        loads[i].wait()
        lax.fori_loop(8 * i, 8 * i + 8, add_up, 0)

    pad = jnp.zeros((16, 128), jnp.float32)
    for b in range(8):
        s = sums[:, 0, 128 * b : 128 * b + 128]
        t = jnp.concatenate([s, pad, pltpu.roll(s, 112, 1), pad], axis=0).T
        for q in range(4):
            sums_send[4 * b + q] = t[32 * q : 32 * q + 16]
    for offset in OFFSETS + ((0, 0, 1),):
        d = peer(offset)
        pltpu.make_async_remote_copy(
            src_ref=sums_send.at[d],
            dst_ref=sums_recv.at[me],
            send_sem=sums_send_sem,
            recv_sem=sums_recv_sem,
            device_id={"zero": d},
            device_id_type=MESH,
        ).start()
        pltpu.make_async_remote_copy(
            src_ref=part_send,
            dst_ref=part_recv.at[me],
            send_sem=part_send_sem,
            recv_sem=part_recv_sem,
            device_id={"zero": d},
            device_id_type=MESH,
        ).start()
    sums_recv[me] = sums_send[me]

    def code_and_send(c, _):
        lax.fori_loop(0, PER, code_pair(c), 0)
        send_chunk(c)
        return 0

    lax.fori_loop(1, CHUNKS, code_and_send, 0)

    others = pl.ds(0, ZERO - 1)
    pltpu.make_async_copy(
        sums_recv.at[others], sums_recv.at[others], sums_recv_sem
    ).wait()
    total = sums_recv[0]
    for s in range(1, ZERO):
        total = total + sums_recv[s]
    root = jnp.sqrt(jnp.concatenate([total] + [jnp.zeros((112, 128), jnp.float32)], 0).T)
    first, second = root[0:48], pltpu.roll(root[64:112], 16, 1)
    lane = lax.broadcasted_iota(jnp.int32, (48, 128), 1)
    scale[...] = jnp.where(lane < 16, first, second)[:, 0:32]

    for n in range(16):
        rows = jnp.concatenate(
            [sums_recv[:, n, :], jnp.zeros((96, 128), jnp.float32)], axis=0
        ).T
        whole = jnp.sum(rows, axis=1, keepdims=True)
        ratio = jnp.sqrt(rows) * lax.rsqrt(whole) * (1.0 / UP)
        table[:, n, :] = ratio[0:64]
        table[:, n + 16, :] = ratio[64:128]

    half = lax.broadcasted_iota(jnp.int32, (32, 128), 1) < 64

    def decode_pair(c):
        def go(k, _):
            p = c * PER + k
            rows = pl.ds(pl.multiple_of(32 * k, 32), 32)
            f0 = table[2 * p]
            f1 = table[2 * p + 1]
            for t in range(16):
                columns = slice(128 * t, 128 * t + 128)
                a = recv[c, 2 * t, rows, :].astype(jnp.float32)
                b = recv[c, 2 * t + 1, rows, :].astype(jnp.float32)
                for e, f, u in (
                    (0, f0, jnp.where(half, a, pltpu.roll(b, 64, 1))),
                    (1, f1, jnp.where(half, pltpu.roll(a, 64, 1), b)),
                ):
                    g = jnp.where(
                        half,
                        jnp.broadcast_to(f[:, 2 * t : 2 * t + 1], (32, 128)),
                        jnp.broadcast_to(f[:, 2 * t + 1 : 2 * t + 2], (32, 128)),
                    )
                    m = jnp.exp(jnp.log(jnp.abs(u)) * (1.0 / POWER))
                    v = jnp.where(u < 0.0, -m, m) * g
                    out[2 * p + e, :, columns] = v.astype(jnp.bfloat16)
            return 0

        return go

    pltpu.make_async_copy(
        part_recv.at[others], part_recv.at[others], part_recv_sem
    ).wait()
    mine = pl.ds(pl.multiple_of(16 * bank, 16), 16)
    for t in range(16):
        a = part_recv[2 * t].astype(jnp.float32)
        b = part_recv[2 * t + 1].astype(jnp.float32)
        low = half[0:8]
        block = jnp.concatenate(
            [
                jnp.where(low, a, pltpu.roll(b, 64, 1)),
                jnp.where(low, pltpu.roll(a, 64, 1), b),
            ],
            axis=0,
        )
        router[mine, 128 * t : 128 * t + 128] = block.astype(jnp.bfloat16)
    rows_out = []
    for i in range(1, 4):
        copy = pltpu.make_async_remote_copy(
            src_ref=router.at[mine],
            dst_ref=router.at[mine],
            send_sem=row_send_sem,
            recv_sem=row_recv_sem,
            device_id={"bank": lax.rem(bank + i, 4)},
            device_id_type=MESH,
        )
        copy.start()
        rows_out.append(copy)

    def receive(c, _):
        pltpu.make_async_copy(
            recv.at[c, others], recv.at[c, others], recv_sem.at[c]
        ).wait()
        lax.fori_loop(0, PER, decode_pair(c), 0)
        return 0

    lax.fori_loop(0, CHUNKS, receive, 0)

    three = pl.ds(0, 48)
    pltpu.make_async_copy(router.at[three], router.at[three], row_recv_sem).wait()
    pltpu.make_async_copy(router.at[three], router.at[three], row_send_sem).wait()
    pltpu.make_async_copy(
        sums_send.at[others], sums_send.at[others], sums_send_sem
    ).wait()
    pltpu.make_async_copy(
        part_recv.at[others], part_recv.at[others], part_send_sem
    ).wait()

    def drain(c, _):
        pltpu.make_async_copy(
            send.at[c, others], send.at[c, others], send_sem.at[c]
        ).wait()
        return 0

    lax.fori_loop(0, CHUNKS, drain, 0)


def hand_out(out, scale, router, gate, up, down, sg, su, sd, served, sem):
    copies = [pltpu.make_async_copy(router, served, sem.at[0])]
    for a, (big, small) in enumerate(((gate, sg), (up, su), (down, sd))):
        part = pl.ds(16 * a, 16)
        copies.append(pltpu.make_async_copy(out.at[part], big, sem.at[2 * a + 1]))
        copies.append(pltpu.make_async_copy(scale.at[part], small, sem.at[2 * a + 2]))
    for copy in copies:
        copy.start()
    for copy in copies:
        copy.wait()


def body(gate, up, down, weight, gain):
    vmem = pl.BlockSpec(memory_space=pltpu.VMEM)
    hbm = pl.BlockSpec(memory_space=pltpu.HBM)
    f32, bf16 = jnp.float32, jnp.bfloat16
    dma, plain = pltpu.SemaphoreType.DMA, pltpu.SemaphoreType.REGULAR
    out, scale, router = pl.pallas_call(
        exchange,
        name="exchange",
        out_shape=(
            pltpu.VMEM((48, 32, 2048), bf16),
            pltpu.VMEM((48, 32), f32),
            pltpu.VMEM((64, 2048), bf16),
        ),
        in_specs=[hbm, hbm, hbm, vmem, vmem],
        out_specs=(vmem, vmem, vmem),
        scratch_shapes=[
            pltpu.VMEM((48, 64, 1024), f32),
            pltpu.VMEM((CHUNKS, ZERO, ROWS, 128), bf16),
            pltpu.VMEM((CHUNKS, ZERO, ROWS, 128), bf16),
            pltpu.VMEM((48, 1, 1024), f32),
            pltpu.VMEM((ZERO, 16, 128), f32),
            pltpu.VMEM((ZERO, 16, 128), f32),
            pltpu.VMEM((64, 32, 128), f32),
            pltpu.VMEM((8, 128), bf16),
            pltpu.VMEM((ZERO, 8, 128), bf16),
            dma((6,)),
            dma((CHUNKS,)),
            dma((CHUNKS,)),
            dma,
            dma,
            dma,
            dma,
            dma,
            dma,
        ],
        compiler_params=pltpu.CompilerParams(
            collective_id=0, has_side_effects=True, vmem_limit_bytes=48 * 2**20
        ),
    )(gate, up, jnp.swapaxes(down, 1, 2), weight.T, gain.reshape(1, 64))
    half = jax.ShapeDtypeStruct((16, 32, 2048), bf16)
    few = jax.ShapeDtypeStruct((16, 32), f32)
    gate, up, down, sg, su, sd, served = pl.pallas_call(
        hand_out,
        name="hand_out",
        out_shape=(half, half, half, few, few, few, jax.ShapeDtypeStruct((64, 2048), bf16)),
        in_specs=[pl.BlockSpec(memory_space=pl.ANY)] * 3,
        out_specs=(hbm,) * 7,
        scratch_shapes=[dma((7,))],
    )(out, scale, router)
    return (
        jnp.swapaxes(gate, 1, 2),
        jnp.swapaxes(up, 1, 2),
        down,
        sg,
        su,
        sd,
        served.T,
    )


def solution(mesh):
    return jax.shard_map(
        body,
        mesh=mesh,
        in_specs=(
            P("bank", "zero", None),
            P("bank", "zero", None),
            P("bank", None, "zero"),
            P("zero", "bank"),
            P("zero"),
        ),
        out_specs=(
            P("bank", None, "zero"),
            P("bank", None, "zero"),
            P("bank", "zero", None),
            P("bank", "zero"),
            P("bank", "zero"),
            P("bank", "zero"),
            P(),
        ),
        check_vma=False,
    )
```

```python
import jax
import jax.numpy as jnp
from jax import lax
from jax.experimental import pallas as pl
from jax.experimental.pallas import tpu as pltpu
from jax.sharding import PartitionSpec as P

MESH = pl.DeviceIdType.MESH
ZERO = 32
CHUNKS = 6
PAIRS = 24
PER = PAIRS // CHUNKS
ROWS = PER * 32
POWER = 20
UP = 2.0**6.25
ORDER = (
    (0, 1), (3, 0), (2, 3), (1, 1), (3, 3), (0, 2), (1, 0), (3, 1),
    (1, 3), (2, 2), (2, 0), (0, 3), (1, 2), (3, 2), (2, 1),
)
OFFSETS = tuple((z, x, c) for z, x in ORDER for c in (0, 1))


def exchange(
    gate, up, down, weight, gain,
    out, scale, router,
    xin, send, recv, sums, sums_send, sums_recv, table, part_send, part_recv,
    in_sem, send_sem, recv_sem, sums_send_sem, sums_recv_sem,
    part_send_sem, part_recv_sem, row_send_sem, row_recv_sem,
):
    me = lax.axis_index("zero")
    bank = lax.axis_index("bank")
    mz, mx, mc = lax.div(me, 8), lax.rem(lax.div(me, 2), 4), lax.rem(me, 2)

    def peer(offset):
        z, x, c = offset
        return (
            lax.rem(mz + z, 4) * 8 + lax.rem(mx + x, 4) * 2 + lax.rem(mc + c, 2)
        )

    loads = []
    for a, ref in enumerate((gate, up, down)):
        for h in range(2):
            copy = pltpu.make_async_copy(
                ref.at[pl.ds(8 * h, 8)],
                xin.at[pl.ds(16 * a + 8 * h, 8)],
                in_sem.at[2 * a + h],
            )
            copy.start()
            loads.append(copy)

    barrier = pltpu.get_barrier_semaphore()

    def greet(i, _):
        pl.semaphore_signal(
            barrier,
            inc=1,
            device_id={"zero": lax.rem(me + i, ZERO)},
            device_id_type=MESH,
        )
        return 0

    lax.fori_loop(1, ZERO, greet, 0)
    for i in range(1, 4):
        pl.semaphore_signal(
            barrier,
            inc=1,
            device_id={"bank": lax.rem(bank + i, 4)},
            device_id_type=MESH,
        )

    part = (weight[...] * gain[...]).astype(jnp.bfloat16)
    packed = jnp.concatenate([part[0:8], part[8:16]], axis=1)
    part_send[...] = packed
    part_recv[me] = packed

    def add_up(e, _):
        x = xin[e]
        sums[e] = jnp.sum(x * x, axis=0, keepdims=True)
        return 0

    def code_pair(c):
        def go(k, _):
            p = c * PER + k
            for b in range(8):
                columns = slice(128 * b, 128 * b + 128)
                halves = []
                for e in range(2):
                    s = sums[2 * p + e, :, columns]
                    r = jnp.where(s > 0.0, lax.rsqrt(s) * UP, 0.0)
                    halves.append(xin[2 * p + e, :, columns] * r)
                y = jnp.concatenate(halves, axis=0).T
                y2 = y * y
                y4 = y2 * y2
                y8 = y4 * y4
                y20 = y8 * y8 * y4
                u = jnp.where(y < 0.0, -y20, y20).astype(jnp.bfloat16)
                for q in range(4):
                    send[c, 4 * b + q, pl.ds(pl.multiple_of(32 * k, 32), 32), :] = u[
                        32 * q : 32 * q + 32
                    ]
            return 0

        return go

    def send_chunk(c):
        for offset in OFFSETS:
            d = peer(offset)
            pltpu.make_async_remote_copy(
                src_ref=send.at[c, d],
                dst_ref=recv.at[c, me],
                send_sem=send_sem.at[c],
                recv_sem=recv_sem.at[c],
                device_id={"zero": d},
                device_id_type=MESH,
            ).start()
        d = peer((0, 0, 1))
        pltpu.make_async_remote_copy(
            src_ref=send.at[c, d],
            dst_ref=recv.at[c, me],
            send_sem=send_sem.at[c],
            recv_sem=recv_sem.at[c],
            device_id={"zero": d},
            device_id_type=MESH,
        ).start()
        recv[c, me] = send[c, me]

    loads[0].wait()
    lax.fori_loop(0, 8, add_up, 0)
    lax.fori_loop(0, PER, code_pair(0), 0)
    pl.semaphore_wait(barrier, ZERO - 1 + 3)
    send_chunk(0)

    for i in range(1, 6):
        loads[i].wait()
        lax.fori_loop(8 * i, 8 * i + 8, add_up, 0)

    pad = jnp.zeros((16, 128), jnp.float32)
    for b in range(8):
        s = sums[:, 0, 128 * b : 128 * b + 128]
        t = jnp.concatenate([s, pad, pltpu.roll(s, 112, 1), pad], axis=0).T
        for q in range(4):
            sums_send[4 * b + q] = t[32 * q : 32 * q + 16]
    for offset in OFFSETS + ((0, 0, 1),):
        d = peer(offset)
        pltpu.make_async_remote_copy(
            src_ref=sums_send.at[d],
            dst_ref=sums_recv.at[me],
            send_sem=sums_send_sem,
            recv_sem=sums_recv_sem,
            device_id={"zero": d},
            device_id_type=MESH,
        ).start()
        pltpu.make_async_remote_copy(
            src_ref=part_send,
            dst_ref=part_recv.at[me],
            send_sem=part_send_sem,
            recv_sem=part_recv_sem,
            device_id={"zero": d},
            device_id_type=MESH,
        ).start()
    sums_recv[me] = sums_send[me]

    def code_and_send(c, _):
        lax.fori_loop(0, PER, code_pair(c), 0)
        send_chunk(c)
        return 0

    lax.fori_loop(1, CHUNKS, code_and_send, 0)

    others = pl.ds(0, ZERO - 1)
    pltpu.make_async_copy(
        sums_recv.at[others], sums_recv.at[others], sums_recv_sem
    ).wait()
    total = sums_recv[0]
    for s in range(1, ZERO):
        total = total + sums_recv[s]
    root = jnp.sqrt(jnp.concatenate([total] + [jnp.zeros((112, 128), jnp.float32)], 0).T)
    first, second = root[0:48], pltpu.roll(root[64:112], 16, 1)
    lane = lax.broadcasted_iota(jnp.int32, (48, 128), 1)
    scale[...] = jnp.where(lane < 16, first, second)[:, 0:32]

    for n in range(16):
        rows = jnp.concatenate(
            [sums_recv[:, n, :], jnp.zeros((96, 128), jnp.float32)], axis=0
        ).T
        whole = jnp.sum(rows, axis=1, keepdims=True)
        ratio = jnp.sqrt(rows) * lax.rsqrt(whole) * (1.0 / UP)
        table[:, n, :] = ratio[0:64]
        table[:, n + 16, :] = ratio[64:128]

    half = lax.broadcasted_iota(jnp.int32, (32, 128), 1) < 64

    def decode_pair(c):
        def go(k, _):
            p = c * PER + k
            rows = pl.ds(pl.multiple_of(32 * k, 32), 32)
            f0 = table[2 * p]
            f1 = table[2 * p + 1]
            for t in range(16):
                columns = slice(128 * t, 128 * t + 128)
                a = recv[c, 2 * t, rows, :].astype(jnp.float32)
                b = recv[c, 2 * t + 1, rows, :].astype(jnp.float32)
                for e, f, u in (
                    (0, f0, jnp.where(half, a, pltpu.roll(b, 64, 1))),
                    (1, f1, jnp.where(half, pltpu.roll(a, 64, 1), b)),
                ):
                    g = jnp.where(
                        half,
                        jnp.broadcast_to(f[:, 2 * t : 2 * t + 1], (32, 128)),
                        jnp.broadcast_to(f[:, 2 * t + 1 : 2 * t + 2], (32, 128)),
                    )
                    m = jnp.exp(jnp.log(jnp.abs(u)) * (1.0 / POWER))
                    v = jnp.where(u < 0.0, -m, m) * g
                    out[2 * p + e, :, columns] = v.astype(jnp.bfloat16)
            return 0

        return go

    pltpu.make_async_copy(
        part_recv.at[others], part_recv.at[others], part_recv_sem
    ).wait()
    mine = pl.ds(pl.multiple_of(16 * bank, 16), 16)
    for t in range(16):
        a = part_recv[2 * t].astype(jnp.float32)
        b = part_recv[2 * t + 1].astype(jnp.float32)
        low = half[0:8]
        block = jnp.concatenate(
            [
                jnp.where(low, a, pltpu.roll(b, 64, 1)),
                jnp.where(low, pltpu.roll(a, 64, 1), b),
            ],
            axis=0,
        )
        router[mine, 128 * t : 128 * t + 128] = block.astype(jnp.bfloat16)
    rows_out = []
    for i in range(1, 4):
        copy = pltpu.make_async_remote_copy(
            src_ref=router.at[mine],
            dst_ref=router.at[mine],
            send_sem=row_send_sem,
            recv_sem=row_recv_sem,
            device_id={"bank": lax.rem(bank + i, 4)},
            device_id_type=MESH,
        )
        copy.start()
        rows_out.append(copy)

    def receive(c, _):
        pltpu.make_async_copy(
            recv.at[c, others], recv.at[c, others], recv_sem.at[c]
        ).wait()
        lax.fori_loop(0, PER, decode_pair(c), 0)
        return 0

    lax.fori_loop(0, CHUNKS, receive, 0)

    three = pl.ds(0, 48)
    pltpu.make_async_copy(router.at[three], router.at[three], row_recv_sem).wait()
    pltpu.make_async_copy(router.at[three], router.at[three], row_send_sem).wait()
    pltpu.make_async_copy(
        sums_send.at[others], sums_send.at[others], sums_send_sem
    ).wait()
    pltpu.make_async_copy(
        part_recv.at[others], part_recv.at[others], part_send_sem
    ).wait()

    def drain(c, _):
        pltpu.make_async_copy(
            send.at[c, others], send.at[c, others], send_sem.at[c]
        ).wait()
        return 0

    lax.fori_loop(0, CHUNKS, drain, 0)


def hand_out(out, scale, router, gate, up, down, sg, su, sd, served, sem):
    copies = [pltpu.make_async_copy(router, served, sem.at[0])]
    for a, (big, small) in enumerate(((gate, sg), (up, su), (down, sd))):
        part = pl.ds(16 * a, 16)
        copies.append(pltpu.make_async_copy(out.at[part], big, sem.at[2 * a + 1]))
        copies.append(pltpu.make_async_copy(scale.at[part], small, sem.at[2 * a + 2]))
    for copy in copies:
        copy.start()
    for copy in copies:
        copy.wait()


def body(gate, up, down, weight, gain):
    vmem = pl.BlockSpec(memory_space=pltpu.VMEM)
    hbm = pl.BlockSpec(memory_space=pltpu.HBM)
    f32, bf16 = jnp.float32, jnp.bfloat16
    dma, plain = pltpu.SemaphoreType.DMA, pltpu.SemaphoreType.REGULAR
    out, scale, router = pl.pallas_call(
        exchange,
        name="exchange",
        out_shape=(
            pltpu.VMEM((48, 32, 2048), bf16),
            pltpu.VMEM((48, 32), f32),
            pltpu.VMEM((64, 2048), bf16),
        ),
        in_specs=[hbm, hbm, hbm, vmem, vmem],
        out_specs=(vmem, vmem, vmem),
        scratch_shapes=[
            pltpu.VMEM((48, 64, 1024), f32),
            pltpu.VMEM((CHUNKS, ZERO, ROWS, 128), bf16),
            pltpu.VMEM((CHUNKS, ZERO, ROWS, 128), bf16),
            pltpu.VMEM((48, 1, 1024), f32),
            pltpu.VMEM((ZERO, 16, 128), f32),
            pltpu.VMEM((ZERO, 16, 128), f32),
            pltpu.VMEM((64, 32, 128), f32),
            pltpu.VMEM((8, 128), bf16),
            pltpu.VMEM((ZERO, 8, 128), bf16),
            dma((6,)),
            dma((CHUNKS,)),
            dma((CHUNKS,)),
            dma,
            dma,
            dma,
            dma,
            dma,
            dma,
        ],
        compiler_params=pltpu.CompilerParams(
            collective_id=0, has_side_effects=True, vmem_limit_bytes=48 * 2**20
        ),
    )(gate, up, jnp.swapaxes(down, 1, 2), weight.T, gain.reshape(1, 64))
    half = jax.ShapeDtypeStruct((16, 32, 2048), bf16)
    few = jax.ShapeDtypeStruct((16, 32), f32)
    gate, up, down, sg, su, sd, served = pl.pallas_call(
        hand_out,
        name="hand_out",
        out_shape=(half, half, half, few, few, few, jax.ShapeDtypeStruct((64, 2048), bf16)),
        in_specs=[vmem] * 3,
        out_specs=(hbm,) * 7,
        scratch_shapes=[dma((7,))],
        compiler_params=pltpu.CompilerParams(vmem_limit_bytes=16 * 2**20),
    )(*(pltpu.with_memory_space_constraint(a, pltpu.VMEM) for a in (out, scale, router)))
    return (
        jnp.swapaxes(gate, 1, 2),
        jnp.swapaxes(up, 1, 2),
        down,
        sg,
        su,
        sd,
        served.T,
    )


def solution(mesh):
    return jax.shard_map(
        body,
        mesh=mesh,
        in_specs=(
            P("bank", "zero", None),
            P("bank", "zero", None),
            P("bank", None, "zero"),
            P("zero", "bank"),
            P("zero"),
        ),
        out_specs=(
            P("bank", None, "zero"),
            P("bank", None, "zero"),
            P("bank", "zero", None),
            P("bank", "zero"),
            P("bank", "zero"),
            P("bank", "zero"),
            P(),
        ),
        check_vma=False,
    )
```

```python
import jax
import jax.numpy as jnp
from jax import lax
from jax.experimental import pallas as pl
from jax.experimental.pallas import tpu as pltpu
from jax.sharding import PartitionSpec as P

MESH = pl.DeviceIdType.MESH
CHUNKS = 6
PAIRS = 24
PER = PAIRS // CHUNKS // 2
ROWS = PER * 32
POWER = 20
UP = 2.0**6.25


def exchange(
    gate, up, down, weight, gain,
    out, scale, router,
    xin, send, relay, recv, sums, sums_send, sums_relay, sums_recv, table, parts,
    in_sem, send_sem, relay_sem, pass_sem, recv_sem,
    sums_send_sem, sums_relay_sem, sums_pass_sem, sums_recv_sem,
    parts_send_sem, parts_recv_sem, row_send_sem, row_recv_sem,
):
    me = lax.axis_index("zero")
    bank = lax.axis_index("bank")
    mz, mx, mc = lax.div(me, 8), lax.rem(lax.div(me, 2), 4), lax.rem(me, 2)
    mate = 1 - mc

    def turn(place, i):
        return lax.rem(place + i, 4)

    def device(z, x, c):
        return z * 8 + x * 2 + c

    def put(src, dst, sent, arrived, z, x, c):
        pltpu.make_async_remote_copy(
            src_ref=src,
            dst_ref=dst,
            send_sem=sent,
            recv_sem=arrived,
            device_id={"zero": device(z, x, c)},
            device_id_type=MESH,
        ).start()

    def wait(ref, sem):
        pltpu.make_async_copy(ref, ref, sem).wait()

    loads = []
    for a, ref in enumerate((gate, up, down)):
        for h in range(2):
            copy = pltpu.make_async_copy(
                ref.at[pl.ds(8 * h, 8)],
                xin.at[pl.ds(16 * a + 8 * h, 8)],
                in_sem.at[2 * a + h],
            )
            copy.start()
            loads.append(copy)

    barrier = pltpu.get_barrier_semaphore()

    def greet(**where):
        pl.semaphore_signal(
            barrier, inc=1, device_id=where, device_id_type=MESH
        )

    greet(zero=device(mz, mx, mate))
    for i in (1, 3, 2):
        for c in range(2):
            greet(zero=device(turn(mz, i), mx, c))
            greet(zero=device(mz, turn(mx, i), c))
        greet(bank=turn(bank, i))

    part = (weight[...] * gain[...]).astype(jnp.bfloat16)
    parts[mc, mz, mx] = jnp.concatenate([part[0:8], part[8:16]], axis=1)

    def add_up(e, _):
        x = xin[e]
        sums[e] = jnp.sum(x * x, axis=0, keepdims=True)
        return 0

    def code_pair(c, h):
        def go(k, _):
            p = (2 * c + h) * PER + k
            rows = pl.ds(pl.multiple_of(32 * k, 32), 32)
            for b in range(8):
                columns = slice(128 * b, 128 * b + 128)
                halves = []
                for e in range(2):
                    s = sums[2 * p + e, :, columns]
                    r = jnp.where(s > 0.0, lax.rsqrt(s) * UP, 0.0)
                    halves.append(xin[2 * p + e, :, columns] * r)
                y = jnp.concatenate(halves, axis=0).T
                y2 = y * y
                y4 = y2 * y2
                y8 = y4 * y4
                y20 = y8 * y8 * y4
                u = jnp.where(y < 0.0, -y20, y20).astype(jnp.bfloat16)
                for q in range(4):
                    z, x, d = b // 2, b % 2 * 2 + q // 2, q % 2
                    first, second = ((x, z), (z, x))[h]
                    send[h, c, first, 2 * second + d, rows, :] = u[32 * q : 32 * q + 32]
            return 0

        return go

    def code(c):
        for h in range(2):
            lax.fori_loop(0, PER, code_pair(c, h), 0)

    def leave(c):
        for i in (1, 3, 2):
            x, z = turn(mx, i), turn(mz, i)
            put(send.at[0, c, x], relay.at[0, c, mx], send_sem, relay_sem.at[0, c], mz, x, mc)
            put(send.at[1, c, z], relay.at[1, c, mz], send_sem, relay_sem.at[1, c], z, mx, mc)
        relay[0, c, mx] = send[0, c, mx]
        relay[1, c, mz] = send[1, c, mz]

    four = pl.ds(0, 4)
    three = pl.ds(0, 3)

    def go_on(c):
        for h in range(2):
            wait(relay.at[h, c, three], relay_sem.at[h, c])
        at_z, at_x = 2 * mz + mc, 2 * mx + mc
        for i in (1, 3, 2):
            for d in range(2):
                x, z = turn(mx, i), turn(mz, i)
                put(relay.at[0, c, four, 2 * z + d], recv.at[0, c, at_z], pass_sem, recv_sem.at[0, c], z, mx, d)
                put(relay.at[1, c, four, 2 * x + d], recv.at[1, c, at_x], pass_sem, recv_sem.at[1, c], mz, x, d)
        put(relay.at[0, c, four, 2 * mz + mate], recv.at[0, c, at_z], pass_sem, recv_sem.at[0, c], mz, mx, mate)
        put(relay.at[1, c, four, 2 * mx + mate], recv.at[1, c, at_x], pass_sem, recv_sem.at[1, c], mz, mx, mate)
        recv[0, c, at_z] = relay[0, c, :, at_z]
        recv[1, c, at_x] = relay[1, c, :, at_x]

    loads[0].wait()
    lax.fori_loop(0, 8, add_up, 0)
    code(0)
    pl.semaphore_wait(barrier, 16)
    leave(0)

    for i in range(1, 6):
        loads[i].wait()
        lax.fori_loop(8 * i, 8 * i + 8, add_up, 0)

    pad = jnp.zeros((16, 128), jnp.float32)
    for b in range(8):
        s = sums[:, 0, 128 * b : 128 * b + 128]
        t = jnp.concatenate([s, pad, pltpu.roll(s, 112, 1), pad], axis=0).T
        for q in range(4):
            z, x, d = b // 2, b % 2 * 2 + q // 2, q % 2
            sums_send[x, 2 * z + d] = t[32 * q : 32 * q + 16]
    for i in (1, 3, 2):
        x = turn(mx, i)
        put(sums_send.at[x], sums_relay.at[mx], sums_send_sem, sums_relay_sem, mz, x, mc)
        put(parts.at[mc, mz, mx], parts.at[mc, mz, mx], parts_send_sem.at[0], parts_recv_sem.at[0], mz, x, mc)
    sums_relay[mx] = sums_send[mx]

    code(1)
    leave(1)

    wait(sums_relay.at[three], sums_relay_sem)
    wait(parts.at[0, 0, three], parts_recv_sem.at[0])
    at_z = 2 * mz + mc
    for i in (1, 3, 2):
        z = turn(mz, i)
        for d in range(2):
            put(sums_relay.at[four, 2 * z + d], sums_recv.at[at_z], sums_pass_sem, sums_recv_sem, z, mx, d)
        put(parts.at[mc, mz], parts.at[mc, mz], parts_send_sem.at[1], parts_recv_sem.at[1], z, mx, mc)
    put(sums_relay.at[four, 2 * mz + mate], sums_recv.at[at_z], sums_pass_sem, sums_recv_sem, mz, mx, mate)
    sums_recv[at_z] = sums_relay[:, at_z]

    go_on(0)
    code(2)
    leave(2)

    wait(sums_recv.at[pl.ds(0, 7)], sums_recv_sem)
    total = jnp.zeros((16, 128), jnp.float32)
    for s in range(32):
        total = total + sums_recv[s // 4, s % 4]
    root = jnp.sqrt(jnp.concatenate([total] + [jnp.zeros((112, 128), jnp.float32)], 0).T)
    first, second = root[0:48], pltpu.roll(root[64:112], 16, 1)
    lane = lax.broadcasted_iota(jnp.int32, (48, 128), 1)
    scale[...] = jnp.where(lane < 16, first, second)[:, 0:32]

    for n in range(16):
        rows = jnp.concatenate(
            [
                sums_recv[:, :, n, :].reshape(32, 128),
                jnp.zeros((96, 128), jnp.float32),
            ],
            axis=0,
        ).T
        whole = jnp.sum(rows, axis=1, keepdims=True)
        ratio = jnp.sqrt(rows) * lax.rsqrt(whole) * (1.0 / UP)
        table[:, n, :] = ratio[0:64]
        table[:, n + 16, :] = ratio[64:128]

    half = lax.broadcasted_iota(jnp.int32, (32, 128), 1) < 64

    def decode_pair(c, h):
        def go(k, _):
            p = (2 * c + h) * PER + k
            rows = pl.ds(pl.multiple_of(32 * k, 32), 32)
            f0 = table[2 * p]
            f1 = table[2 * p + 1]
            for t in range(16):
                z, x = t // 4, t % 4
                one, two = ((z, x), (x, z))[h]
                left, right = 8 * z + x, 8 * z + 4 + x
                columns = slice(128 * t, 128 * t + 128)
                a = recv[h, c, 2 * one, two, rows, :].astype(jnp.float32)
                b = recv[h, c, 2 * one + 1, two, rows, :].astype(jnp.float32)
                for e, f, u in (
                    (0, f0, jnp.where(half, a, pltpu.roll(b, 64, 1))),
                    (1, f1, jnp.where(half, pltpu.roll(a, 64, 1), b)),
                ):
                    g = jnp.where(
                        half,
                        jnp.broadcast_to(f[:, left : left + 1], (32, 128)),
                        jnp.broadcast_to(f[:, right : right + 1], (32, 128)),
                    )
                    m = jnp.exp(jnp.log(jnp.abs(u)) * (1.0 / POWER))
                    v = jnp.where(u < 0.0, -m, m) * g
                    out[2 * p + e, :, columns] = v.astype(jnp.bfloat16)
            return 0

        return go

    def decode(c):
        for h in range(2):
            wait(recv.at[h, c, pl.ds(0, 7)], recv_sem.at[h, c])
            lax.fori_loop(0, PER, decode_pair(c, h), 0)

    wait(parts.at[0, three], parts_recv_sem.at[1])
    put(parts.at[mc], parts.at[mc], parts_send_sem.at[2], parts_recv_sem.at[2], mz, mx, mate)

    def step(c, _):
        go_on(c)

        @pl.when(c < CHUNKS - 2)
        def _():
            code(c + 2)
            leave(c + 2)

        decode(c - 1)
        return 0

    lax.fori_loop(1, CHUNKS - 1, step, 0)

    wait(parts.at[0], parts_recv_sem.at[2])
    mine = pl.ds(pl.multiple_of(16 * bank, 16), 16)
    low = half[0:8]
    for t in range(16):
        z, x = t // 4, t % 4
        a = parts[0, z, x].astype(jnp.float32)
        b = parts[1, z, x].astype(jnp.float32)
        block = jnp.concatenate(
            [
                jnp.where(low, a, pltpu.roll(b, 64, 1)),
                jnp.where(low, pltpu.roll(a, 64, 1), b),
            ],
            axis=0,
        )
        router[mine, 128 * t : 128 * t + 128] = block.astype(jnp.bfloat16)
    for i in range(1, 4):
        pltpu.make_async_remote_copy(
            src_ref=router.at[mine],
            dst_ref=router.at[mine],
            send_sem=row_send_sem,
            recv_sem=row_recv_sem,
            device_id={"bank": turn(bank, i)},
            device_id_type=MESH,
        ).start()

    go_on(CHUNKS - 1)
    decode(CHUNKS - 2)
    rest = pl.ds(0, 48)
    wait(router.at[rest], row_recv_sem)
    wait(router.at[rest], row_send_sem)
    wait(parts.at[0, 0, three], parts_send_sem.at[0])
    wait(parts.at[0, three], parts_send_sem.at[1])
    wait(parts.at[0], parts_send_sem.at[2])
    wait(sums_send.at[three], sums_send_sem)
    wait(sums_recv.at[pl.ds(0, 7)], sums_pass_sem)
    every = pl.ds(0, CHUNKS)
    both = pl.ds(0, 2)
    wait(send.at[both, every, three], send_sem)
    decode(CHUNKS - 1)
    wait(recv.at[both, every, pl.ds(0, 7)], pass_sem)


def hand_out(out, scale, router, gate, up, down, sg, su, sd, served, sem):
    copies = [pltpu.make_async_copy(router, served, sem.at[0])]
    for a, (big, small) in enumerate(((gate, sg), (up, su), (down, sd))):
        part = pl.ds(16 * a, 16)
        copies.append(pltpu.make_async_copy(out.at[part], big, sem.at[2 * a + 1]))
        copies.append(pltpu.make_async_copy(scale.at[part], small, sem.at[2 * a + 2]))
    for copy in copies:
        copy.start()
    for copy in copies:
        copy.wait()


def body(gate, up, down, weight, gain):
    vmem = pl.BlockSpec(memory_space=pltpu.VMEM)
    hbm = pl.BlockSpec(memory_space=pltpu.HBM)
    f32, bf16 = jnp.float32, jnp.bfloat16
    dma = pltpu.SemaphoreType.DMA
    out, scale, router = pl.pallas_call(
        exchange,
        name="exchange",
        out_shape=(
            pltpu.VMEM((48, 32, 2048), bf16),
            pltpu.VMEM((48, 32), f32),
            pltpu.VMEM((64, 2048), bf16),
        ),
        in_specs=[hbm, hbm, hbm, vmem, vmem],
        out_specs=(vmem, vmem, vmem),
        scratch_shapes=[
            pltpu.VMEM((48, 64, 1024), f32),
            pltpu.VMEM((2, CHUNKS, 4, 8, ROWS, 128), bf16),
            pltpu.VMEM((2, CHUNKS, 4, 8, ROWS, 128), bf16),
            pltpu.VMEM((2, CHUNKS, 8, 4, ROWS, 128), bf16),
            pltpu.VMEM((48, 1, 1024), f32),
            pltpu.VMEM((4, 8, 16, 128), f32),
            pltpu.VMEM((4, 8, 16, 128), f32),
            pltpu.VMEM((8, 4, 16, 128), f32),
            pltpu.VMEM((64, 32, 128), f32),
            pltpu.VMEM((2, 4, 4, 8, 128), bf16),
            dma((6,)),
            dma,
            dma((2, CHUNKS)),
            dma,
            dma((2, CHUNKS)),
            dma,
            dma,
            dma,
            dma,
            dma((3,)),
            dma((3,)),
            dma,
            dma,
        ],
        compiler_params=pltpu.CompilerParams(
            collective_id=0, has_side_effects=True, vmem_limit_bytes=48 * 2**20
        ),
    )(gate, up, jnp.swapaxes(down, 1, 2), weight.T, gain.reshape(1, 64))
    half = jax.ShapeDtypeStruct((16, 32, 2048), bf16)
    few = jax.ShapeDtypeStruct((16, 32), f32)
    gate, up, down, sg, su, sd, served = pl.pallas_call(
        hand_out,
        name="hand_out",
        out_shape=(half, half, half, few, few, few, jax.ShapeDtypeStruct((64, 2048), bf16)),
        in_specs=[vmem] * 3,
        out_specs=(hbm,) * 7,
        scratch_shapes=[dma((7,))],
        compiler_params=pltpu.CompilerParams(vmem_limit_bytes=16 * 2**20),
    )(*(pltpu.with_memory_space_constraint(a, pltpu.VMEM) for a in (out, scale, router)))
    return (
        jnp.swapaxes(gate, 1, 2),
        jnp.swapaxes(up, 1, 2),
        down,
        sg,
        su,
        sd,
        served.T,
    )


def solution(mesh):
    return jax.shard_map(
        body,
        mesh=mesh,
        in_specs=(
            P("bank", "zero", None),
            P("bank", "zero", None),
            P("bank", None, "zero"),
            P("zero", "bank"),
            P("zero"),
        ),
        out_specs=(
            P("bank", None, "zero"),
            P("bank", None, "zero"),
            P("bank", "zero", None),
            P("bank", "zero"),
            P("bank", "zero"),
            P("bank", "zero"),
            P(),
        ),
        check_vma=False,
    )
```

```python
import jax
import jax.numpy as jnp
from jax import lax
from jax.experimental import pallas as pl
from jax.experimental.pallas import tpu as pltpu
from jax.sharding import PartitionSpec as P

MESH = pl.DeviceIdType.MESH
CHUNKS = 12
AHEAD = 4
LOAD = 4
PAIRS = 24
PER = PAIRS // CHUNKS // 2
ROWS = PER * 32
POWER = 20
UP = 2.0**6.25


def exchange(
    gate, up, down, weight, gain,
    out, scale, router,
    xin, send, relay, recv, sums, sums_send, sums_relay, sums_recv, table, parts,
    in_sem, send_sem, relay_sem, pass_sem, recv_sem,
    sums_send_sem, sums_relay_sem, sums_pass_sem, sums_recv_sem,
    parts_send_sem, parts_recv_sem, row_send_sem, row_recv_sem,
):
    me = lax.axis_index("zero")
    bank = lax.axis_index("bank")
    mz, mx, mc = lax.div(me, 8), lax.rem(lax.div(me, 2), 4), lax.rem(me, 2)
    mate = 1 - mc

    def turn(place, i):
        return lax.rem(place + i, 4)

    def device(z, x, c):
        return z * 8 + x * 2 + c

    def put(src, dst, sent, arrived, z, x, c):
        pltpu.make_async_remote_copy(
            src_ref=src,
            dst_ref=dst,
            send_sem=sent,
            recv_sem=arrived,
            device_id={"zero": device(z, x, c)},
            device_id_type=MESH,
        ).start()

    def wait(ref, sem):
        pltpu.make_async_copy(ref, ref, sem).wait()

    loads = [
        pltpu.make_async_copy(
            ref.at[pl.ds(k, LOAD)], xin.at[pl.ds(16 * a + k, LOAD)], in_sem.at[4 * a + k // LOAD]
        )
        for a, ref in enumerate((gate, up, down))
        for k in range(0, 16, LOAD)
    ]
    for copy in loads[:2]:
        copy.start()

    barrier = pltpu.get_barrier_semaphore()

    def greet(**where):
        pl.semaphore_signal(
            barrier, inc=1, device_id=where, device_id_type=MESH
        )

    greet(zero=device(mz, mx, mate))
    for i in (1, 3, 2):
        for c in range(2):
            greet(zero=device(turn(mz, i), mx, c))
            greet(zero=device(mz, turn(mx, i), c))
        greet(bank=turn(bank, i))

    part = (weight[...] * gain[...]).astype(jnp.bfloat16)
    parts[mc, mz, mx] = jnp.concatenate([part[0:8], part[8:16]], axis=1)

    def add_up(e, _):
        x = xin[e]
        sums[e] = jnp.sum(x * x, axis=0, keepdims=True)
        return 0

    def code_pair(c, h):
        def go(k, _):
            p = (2 * c + h) * PER + k
            rows = pl.ds(pl.multiple_of(32 * k, 32), 32)
            for b in range(8):
                columns = slice(128 * b, 128 * b + 128)
                halves = []
                for e in range(2):
                    s = sums[2 * p + e, :, columns]
                    r = jnp.where(s > 0.0, lax.rsqrt(s) * UP, 0.0)
                    halves.append(xin[2 * p + e, :, columns] * r)
                y = jnp.concatenate(halves, axis=0).T
                y2 = y * y
                y4 = y2 * y2
                y8 = y4 * y4
                y20 = y8 * y8 * y4
                u = jnp.where(y < 0.0, -y20, y20).astype(jnp.bfloat16)
                for q in range(4):
                    z, x, d = b // 2, b % 2 * 2 + q // 2, q % 2
                    first, second = ((x, z), (z, x))[h]
                    send[h, c, first, 2 * second + d, rows, :] = u[32 * q : 32 * q + 32]
            return 0

        return go

    def code(c):
        for h in range(2):
            lax.fori_loop(0, PER, code_pair(c, h), 0)

    def leave(c):
        for i in (1, 3, 2):
            x, z = turn(mx, i), turn(mz, i)
            put(send.at[0, c, x], relay.at[0, c, mx], send_sem, relay_sem.at[0, c], mz, x, mc)
            put(send.at[1, c, z], relay.at[1, c, mz], send_sem, relay_sem.at[1, c], z, mx, mc)
        relay[0, c, mx] = send[0, c, mx]
        relay[1, c, mz] = send[1, c, mz]

    four = pl.ds(0, 4)
    three = pl.ds(0, 3)

    def go_on(c):
        for h in range(2):
            wait(relay.at[h, c, three], relay_sem.at[h, c])
        at_z, at_x = 2 * mz + mc, 2 * mx + mc
        for i in (1, 3, 2):
            for d in range(2):
                x, z = turn(mx, i), turn(mz, i)
                put(relay.at[0, c, four, 2 * z + d], recv.at[0, c, at_z], pass_sem, recv_sem.at[0, c], z, mx, d)
                put(relay.at[1, c, four, 2 * x + d], recv.at[1, c, at_x], pass_sem, recv_sem.at[1, c], mz, x, d)
        put(relay.at[0, c, four, 2 * mz + mate], recv.at[0, c, at_z], pass_sem, recv_sem.at[0, c], mz, mx, mate)
        put(relay.at[1, c, four, 2 * mx + mate], recv.at[1, c, at_x], pass_sem, recv_sem.at[1, c], mz, mx, mate)
        recv[0, c, at_z] = relay[0, c, :, at_z]
        recv[1, c, at_x] = relay[1, c, :, at_x]

    loads[0].wait()
    for copy in loads[2:]:
        copy.start()
    lax.fori_loop(0, LOAD, add_up, 0)
    code(0)
    pl.semaphore_wait(barrier, 16)
    leave(0)
    loads[1].wait()
    lax.fori_loop(LOAD, 2 * LOAD, add_up, 0)
    code(1)
    leave(1)

    for i in range(2, 12):
        loads[i].wait()
        lax.fori_loop(LOAD * i, LOAD * i + LOAD, add_up, 0)

    pad = jnp.zeros((16, 128), jnp.float32)
    for b in range(8):
        s = sums[:, 0, 128 * b : 128 * b + 128]
        t = jnp.concatenate([s, pad, pltpu.roll(s, 112, 1), pad], axis=0).T
        for q in range(4):
            z, x, d = b // 2, b % 2 * 2 + q // 2, q % 2
            sums_send[x, 2 * z + d] = t[32 * q : 32 * q + 16]
    for i in (1, 3, 2):
        x = turn(mx, i)
        put(sums_send.at[x], sums_relay.at[mx], sums_send_sem, sums_relay_sem, mz, x, mc)
        put(parts.at[mc, mz, mx], parts.at[mc, mz, mx], parts_send_sem.at[0], parts_recv_sem.at[0], mz, x, mc)
    sums_relay[mx] = sums_send[mx]

    def code_and_leave(c, _):
        code(c)
        leave(c)
        return 0

    lax.fori_loop(2, AHEAD, code_and_leave, 0)
    go_on(0)

    wait(sums_relay.at[three], sums_relay_sem)
    wait(parts.at[0, 0, three], parts_recv_sem.at[0])
    at_z = 2 * mz + mc
    for i in (1, 3, 2):
        z = turn(mz, i)
        for d in range(2):
            put(sums_relay.at[four, 2 * z + d], sums_recv.at[at_z], sums_pass_sem, sums_recv_sem, z, mx, d)
        put(parts.at[mc, mz], parts.at[mc, mz], parts_send_sem.at[1], parts_recv_sem.at[1], z, mx, mc)
    put(sums_relay.at[four, 2 * mz + mate], sums_recv.at[at_z], sums_pass_sem, sums_recv_sem, mz, mx, mate)
    sums_recv[at_z] = sums_relay[:, at_z]

    code_and_leave(AHEAD, 0)
    go_on(1)
    code_and_leave(AHEAD + 1, 0)

    wait(sums_recv.at[pl.ds(0, 7)], sums_recv_sem)
    total = jnp.zeros((16, 128), jnp.float32)
    for s in range(32):
        total = total + sums_recv[s // 4, s % 4]
    root = jnp.sqrt(jnp.concatenate([total] + [jnp.zeros((112, 128), jnp.float32)], 0).T)
    first, second = root[0:48], pltpu.roll(root[64:112], 16, 1)
    lane = lax.broadcasted_iota(jnp.int32, (48, 128), 1)
    scale[...] = jnp.where(lane < 16, first, second)[:, 0:32]

    for n in range(16):
        rows = jnp.concatenate(
            [
                sums_recv[:, :, n, :].reshape(32, 128),
                jnp.zeros((96, 128), jnp.float32),
            ],
            axis=0,
        ).T
        whole = jnp.sum(rows, axis=1, keepdims=True)
        ratio = jnp.sqrt(rows) * lax.rsqrt(whole) * (1.0 / UP)
        table[:, n, :] = ratio[0:64]
        table[:, n + 16, :] = ratio[64:128]

    half = lax.broadcasted_iota(jnp.int32, (32, 128), 1) < 64

    def decode_pair(c, h):
        def go(k, _):
            p = (2 * c + h) * PER + k
            rows = pl.ds(pl.multiple_of(32 * k, 32), 32)
            f0 = table[2 * p]
            f1 = table[2 * p + 1]
            for t in range(16):
                z, x = t // 4, t % 4
                one, two = ((z, x), (x, z))[h]
                left, right = 8 * z + x, 8 * z + 4 + x
                columns = slice(128 * t, 128 * t + 128)
                a = recv[h, c, 2 * one, two, rows, :].astype(jnp.float32)
                b = recv[h, c, 2 * one + 1, two, rows, :].astype(jnp.float32)
                for e, f, u in (
                    (0, f0, jnp.where(half, a, pltpu.roll(b, 64, 1))),
                    (1, f1, jnp.where(half, pltpu.roll(a, 64, 1), b)),
                ):
                    g = jnp.where(
                        half,
                        jnp.broadcast_to(f[:, left : left + 1], (32, 128)),
                        jnp.broadcast_to(f[:, right : right + 1], (32, 128)),
                    )
                    m = jnp.exp(jnp.log(jnp.abs(u)) * (1.0 / POWER))
                    v = jnp.where(u < 0.0, -m, m) * g
                    out[2 * p + e, :, columns] = v.astype(jnp.bfloat16)
            return 0

        return go

    def decode(c):
        for h in range(2):
            wait(recv.at[h, c, pl.ds(0, 7)], recv_sem.at[h, c])
            lax.fori_loop(0, PER, decode_pair(c, h), 0)

    wait(parts.at[0, three], parts_recv_sem.at[1])
    put(parts.at[mc], parts.at[mc], parts_send_sem.at[2], parts_recv_sem.at[2], mz, mx, mate)

    mine = pl.ds(pl.multiple_of(16 * bank, 16), 16)

    def serve_rows():
        wait(parts.at[0], parts_recv_sem.at[2])
        low = half[0:8]
        for t in range(16):
            z, x = t // 4, t % 4
            a = parts[0, z, x].astype(jnp.float32)
            b = parts[1, z, x].astype(jnp.float32)
            block = jnp.concatenate(
                [
                    jnp.where(low, a, pltpu.roll(b, 64, 1)),
                    jnp.where(low, pltpu.roll(a, 64, 1), b),
                ],
                axis=0,
            )
            router[mine, 128 * t : 128 * t + 128] = block.astype(jnp.bfloat16)
        for i in range(1, 4):
            pltpu.make_async_remote_copy(
                src_ref=router.at[mine],
                dst_ref=router.at[mine],
                send_sem=row_send_sem,
                recv_sem=row_recv_sem,
                device_id={"bank": turn(bank, i)},
                device_id_type=MESH,
            ).start()

    def step(c, _):
        go_on(c)

        @pl.when(c < CHUNKS - AHEAD)
        def _():
            code_and_leave(c + AHEAD, 0)

        decode(c - 2)

        @pl.when(c == CHUNKS // 2)
        def _():
            serve_rows()

        return 0

    lax.fori_loop(2, CHUNKS, step, 0)
    decode(CHUNKS - 2)
    rest = pl.ds(0, 48)
    wait(router.at[rest], row_recv_sem)
    wait(router.at[rest], row_send_sem)
    wait(parts.at[0, 0, three], parts_send_sem.at[0])
    wait(parts.at[0, three], parts_send_sem.at[1])
    wait(parts.at[0], parts_send_sem.at[2])
    wait(sums_send.at[three], sums_send_sem)
    wait(sums_recv.at[pl.ds(0, 7)], sums_pass_sem)
    every = pl.ds(0, CHUNKS)
    both = pl.ds(0, 2)
    wait(send.at[both, every, three], send_sem)
    decode(CHUNKS - 1)
    wait(recv.at[both, every, pl.ds(0, 7)], pass_sem)


def hand_out(out, scale, router, gate, up, down, sg, su, sd, served, sem):
    copies = [pltpu.make_async_copy(router, served, sem.at[0])]
    for a, (big, small) in enumerate(((gate, sg), (up, su), (down, sd))):
        part = pl.ds(16 * a, 16)
        copies.append(pltpu.make_async_copy(out.at[part], big, sem.at[2 * a + 1]))
        copies.append(pltpu.make_async_copy(scale.at[part], small, sem.at[2 * a + 2]))
    for copy in copies:
        copy.start()
    for copy in copies:
        copy.wait()


def body(gate, up, down, weight, gain):
    vmem = pl.BlockSpec(memory_space=pltpu.VMEM)
    hbm = pl.BlockSpec(memory_space=pltpu.HBM)
    f32, bf16 = jnp.float32, jnp.bfloat16
    dma = pltpu.SemaphoreType.DMA
    out, scale, router = pl.pallas_call(
        exchange,
        name="exchange",
        out_shape=(
            pltpu.VMEM((48, 32, 2048), bf16),
            pltpu.VMEM((48, 32), f32),
            pltpu.VMEM((64, 2048), bf16),
        ),
        in_specs=[hbm, hbm, hbm, vmem, vmem],
        out_specs=(vmem, vmem, vmem),
        scratch_shapes=[
            pltpu.VMEM((48, 64, 1024), f32),
            pltpu.VMEM((2, CHUNKS, 4, 8, ROWS, 128), bf16),
            pltpu.VMEM((2, CHUNKS, 4, 8, ROWS, 128), bf16),
            pltpu.VMEM((2, CHUNKS, 8, 4, ROWS, 128), bf16),
            pltpu.VMEM((48, 1, 1024), f32),
            pltpu.VMEM((4, 8, 16, 128), f32),
            pltpu.VMEM((4, 8, 16, 128), f32),
            pltpu.VMEM((8, 4, 16, 128), f32),
            pltpu.VMEM((64, 32, 128), f32),
            pltpu.VMEM((2, 4, 4, 8, 128), bf16),
            dma((12,)),
            dma,
            dma((2, CHUNKS)),
            dma,
            dma((2, CHUNKS)),
            dma,
            dma,
            dma,
            dma,
            dma((3,)),
            dma((3,)),
            dma,
            dma,
        ],
        compiler_params=pltpu.CompilerParams(
            collective_id=0, has_side_effects=True, vmem_limit_bytes=48 * 2**20
        ),
    )(gate, up, jnp.swapaxes(down, 1, 2), weight.T, gain.reshape(1, 64))
    half = jax.ShapeDtypeStruct((16, 32, 2048), bf16)
    few = jax.ShapeDtypeStruct((16, 32), f32)
    gate, up, down, sg, su, sd, served = pl.pallas_call(
        hand_out,
        name="hand_out",
        out_shape=(half, half, half, few, few, few, jax.ShapeDtypeStruct((64, 2048), bf16)),
        in_specs=[vmem] * 3,
        out_specs=(hbm,) * 7,
        scratch_shapes=[dma((7,))],
        compiler_params=pltpu.CompilerParams(vmem_limit_bytes=16 * 2**20),
    )(*(pltpu.with_memory_space_constraint(a, pltpu.VMEM) for a in (out, scale, router)))
    return (
        jnp.swapaxes(gate, 1, 2),
        jnp.swapaxes(up, 1, 2),
        down,
        sg,
        su,
        sd,
        served.T,
    )


def solution(mesh):
    return jax.shard_map(
        body,
        mesh=mesh,
        in_specs=(
            P("bank", "zero", None),
            P("bank", "zero", None),
            P("bank", None, "zero"),
            P("zero", "bank"),
            P("zero"),
        ),
        out_specs=(
            P("bank", None, "zero"),
            P("bank", None, "zero"),
            P("bank", "zero", None),
            P("bank", "zero"),
            P("bank", "zero"),
            P("bank", "zero"),
            P(),
        ),
        check_vma=False,
    )
```

```python
import jax
import jax.numpy as jnp
from jax import lax
from jax.experimental import pallas as pl
from jax.experimental.pallas import tpu as pltpu
from jax.sharding import PartitionSpec as P

MESH = pl.DeviceIdType.MESH
CHUNKS = 12
AHEAD = 4
LOAD = 4
PAIRS = 24
PER = PAIRS // CHUNKS // 2
ROWS = PER * 32
POWER = 20
UP = 2.0**6.25


def left_half():
    return lax.broadcasted_iota(jnp.int32, (32, 128), 1) < 64


def decode_pair(recv, table, out, c, h, k, place):
    half = left_half()
    p = (2 * c + h) * PER + k
    rows = pl.ds(pl.multiple_of(32 * k, 32), 32)
    f0 = table[2 * p]
    f1 = table[2 * p + 1]
    for t in range(16):
        z, x = t // 4, t % 4
        one, two = ((z, x), (x, z))[h]
        left, right = 8 * z + x, 8 * z + 4 + x
        columns = slice(128 * t, 128 * t + 128)
        a = recv[h, c, 2 * one, two, rows, :].astype(jnp.float32)
        b = recv[h, c, 2 * one + 1, two, rows, :].astype(jnp.float32)
        for e, f, u in (
            (0, f0, jnp.where(half, a, pltpu.roll(b, 64, 1))),
            (1, f1, jnp.where(half, pltpu.roll(a, 64, 1), b)),
        ):
            g = jnp.where(
                half,
                jnp.broadcast_to(f[:, left : left + 1], (32, 128)),
                jnp.broadcast_to(f[:, right : right + 1], (32, 128)),
            )
            m = jnp.exp(jnp.log(jnp.abs(u)) * (1.0 / POWER))
            v = jnp.where(u < 0.0, -m, m) * g
            out[2 * place + e, :, columns] = v.astype(jnp.bfloat16)


def exchange(
    gate, up, down, weight, gain,
    out, scale, router, recv, table,
    xin, send, relay, sums, sums_send, sums_relay, sums_recv, parts,
    in_sem, send_sem, relay_sem, pass_sem, recv_sem,
    sums_send_sem, sums_relay_sem, sums_pass_sem, sums_recv_sem,
    parts_send_sem, parts_recv_sem, row_send_sem, row_recv_sem,
):
    me = lax.axis_index("zero")
    bank = lax.axis_index("bank")
    mz, mx, mc = lax.div(me, 8), lax.rem(lax.div(me, 2), 4), lax.rem(me, 2)
    mate = 1 - mc

    def turn(place, i):
        return lax.rem(place + i, 4)

    def device(z, x, c):
        return z * 8 + x * 2 + c

    def put(src, dst, sent, arrived, z, x, c):
        pltpu.make_async_remote_copy(
            src_ref=src,
            dst_ref=dst,
            send_sem=sent,
            recv_sem=arrived,
            device_id={"zero": device(z, x, c)},
            device_id_type=MESH,
        ).start()

    def wait(ref, sem):
        pltpu.make_async_copy(ref, ref, sem).wait()

    loads = [
        pltpu.make_async_copy(
            ref.at[pl.ds(k, LOAD)], xin.at[pl.ds(16 * a + k, LOAD)], in_sem.at[4 * a + k // LOAD]
        )
        for a, ref in enumerate((gate, up, down))
        for k in range(0, 16, LOAD)
    ]
    for copy in loads[:2]:
        copy.start()

    barrier = pltpu.get_barrier_semaphore()

    def greet(**where):
        pl.semaphore_signal(
            barrier, inc=1, device_id=where, device_id_type=MESH
        )

    greet(zero=device(mz, mx, mate))
    for i in (1, 3, 2):
        for c in range(2):
            greet(zero=device(turn(mz, i), mx, c))
            greet(zero=device(mz, turn(mx, i), c))
        greet(bank=turn(bank, i))

    part = (weight[...] * gain[...]).astype(jnp.bfloat16)
    parts[mc, mz, mx] = jnp.concatenate([part[0:8], part[8:16]], axis=1)

    def add_up(e, _):
        x = xin[e]
        sums[e] = jnp.sum(x * x, axis=0, keepdims=True)
        return 0

    def code_pair(c, h):
        def go(k, _):
            p = (2 * c + h) * PER + k
            rows = pl.ds(pl.multiple_of(32 * k, 32), 32)
            for b in range(8):
                columns = slice(128 * b, 128 * b + 128)
                halves = []
                for e in range(2):
                    s = sums[2 * p + e, :, columns]
                    r = jnp.where(s > 0.0, lax.rsqrt(s) * UP, 0.0)
                    halves.append(xin[2 * p + e, :, columns] * r)
                y = jnp.concatenate(halves, axis=0).T
                y2 = y * y
                y4 = y2 * y2
                y8 = y4 * y4
                y20 = y8 * y8 * y4
                u = jnp.where(y < 0.0, -y20, y20).astype(jnp.bfloat16)
                for q in range(4):
                    z, x, d = b // 2, b % 2 * 2 + q // 2, q % 2
                    first, second = ((x, z), (z, x))[h]
                    send[h, c, first, 2 * second + d, rows, :] = u[32 * q : 32 * q + 32]
            return 0

        return go

    def code(c):
        for h in range(2):
            lax.fori_loop(0, PER, code_pair(c, h), 0)

    def leave(c):
        for i in (1, 3, 2):
            x, z = turn(mx, i), turn(mz, i)
            put(send.at[0, c, x], relay.at[0, c, mx], send_sem, relay_sem.at[0, c], mz, x, mc)
            put(send.at[1, c, z], relay.at[1, c, mz], send_sem, relay_sem.at[1, c], z, mx, mc)
        relay[0, c, mx] = send[0, c, mx]
        relay[1, c, mz] = send[1, c, mz]

    four = pl.ds(0, 4)
    three = pl.ds(0, 3)

    def go_on(c):
        for h in range(2):
            wait(relay.at[h, c, three], relay_sem.at[h, c])
        at_z, at_x = 2 * mz + mc, 2 * mx + mc
        for i in (1, 3, 2):
            for d in range(2):
                x, z = turn(mx, i), turn(mz, i)
                put(relay.at[0, c, four, 2 * z + d], recv.at[0, c, at_z], pass_sem, recv_sem.at[0, c], z, mx, d)
                put(relay.at[1, c, four, 2 * x + d], recv.at[1, c, at_x], pass_sem, recv_sem.at[1, c], mz, x, d)
        put(relay.at[0, c, four, 2 * mz + mate], recv.at[0, c, at_z], pass_sem, recv_sem.at[0, c], mz, mx, mate)
        put(relay.at[1, c, four, 2 * mx + mate], recv.at[1, c, at_x], pass_sem, recv_sem.at[1, c], mz, mx, mate)
        recv[0, c, at_z] = relay[0, c, :, at_z]
        recv[1, c, at_x] = relay[1, c, :, at_x]

    loads[0].wait()
    for copy in loads[2:]:
        copy.start()
    lax.fori_loop(0, LOAD, add_up, 0)
    code(0)
    pl.semaphore_wait(barrier, 16)
    leave(0)
    loads[1].wait()
    lax.fori_loop(LOAD, 2 * LOAD, add_up, 0)
    code(1)
    leave(1)

    for i in range(2, 12):
        loads[i].wait()
        lax.fori_loop(LOAD * i, LOAD * i + LOAD, add_up, 0)

    pad = jnp.zeros((16, 128), jnp.float32)
    for b in range(8):
        s = sums[:, 0, 128 * b : 128 * b + 128]
        t = jnp.concatenate([s, pad, pltpu.roll(s, 112, 1), pad], axis=0).T
        for q in range(4):
            z, x, d = b // 2, b % 2 * 2 + q // 2, q % 2
            sums_send[x, 2 * z + d] = t[32 * q : 32 * q + 16]
    for i in (1, 3, 2):
        x = turn(mx, i)
        put(sums_send.at[x], sums_relay.at[mx], sums_send_sem, sums_relay_sem, mz, x, mc)
        put(parts.at[mc, mz, mx], parts.at[mc, mz, mx], parts_send_sem.at[0], parts_recv_sem.at[0], mz, x, mc)
    sums_relay[mx] = sums_send[mx]

    def code_and_leave(c, _):
        code(c)
        leave(c)
        return 0

    lax.fori_loop(2, AHEAD, code_and_leave, 0)
    go_on(0)

    wait(sums_relay.at[three], sums_relay_sem)
    wait(parts.at[0, 0, three], parts_recv_sem.at[0])
    at_z = 2 * mz + mc
    for i in (1, 3, 2):
        z = turn(mz, i)
        for d in range(2):
            put(sums_relay.at[four, 2 * z + d], sums_recv.at[at_z], sums_pass_sem, sums_recv_sem, z, mx, d)
        put(parts.at[mc, mz], parts.at[mc, mz], parts_send_sem.at[1], parts_recv_sem.at[1], z, mx, mc)
    put(sums_relay.at[four, 2 * mz + mate], sums_recv.at[at_z], sums_pass_sem, sums_recv_sem, mz, mx, mate)
    sums_recv[at_z] = sums_relay[:, at_z]

    code_and_leave(AHEAD, 0)
    go_on(1)
    code_and_leave(AHEAD + 1, 0)

    wait(sums_recv.at[pl.ds(0, 7)], sums_recv_sem)
    total = jnp.zeros((16, 128), jnp.float32)
    for s in range(32):
        total = total + sums_recv[s // 4, s % 4]
    root = jnp.sqrt(jnp.concatenate([total] + [jnp.zeros((112, 128), jnp.float32)], 0).T)
    first, second = root[0:48], pltpu.roll(root[64:112], 16, 1)
    lane = lax.broadcasted_iota(jnp.int32, (48, 128), 1)
    scale[...] = jnp.where(lane < 16, first, second)[:, 0:32]

    for n in range(16):
        rows = jnp.concatenate(
            [
                sums_recv[:, :, n, :].reshape(32, 128),
                jnp.zeros((96, 128), jnp.float32),
            ],
            axis=0,
        ).T
        whole = jnp.sum(rows, axis=1, keepdims=True)
        ratio = jnp.sqrt(rows) * lax.rsqrt(whole) * (1.0 / UP)
        table[:, n, :] = ratio[0:64]
        table[:, n + 16, :] = ratio[64:128]

    half = left_half()

    def decode(c):
        for h in range(2):
            wait(recv.at[h, c, pl.ds(0, 7)], recv_sem.at[h, c])

            def go(k, _):
                decode_pair(recv, table, out, c, h, k, (2 * c + h) * PER + k)
                return 0

            lax.fori_loop(0, PER, go, 0)

    wait(parts.at[0, three], parts_recv_sem.at[1])
    put(parts.at[mc], parts.at[mc], parts_send_sem.at[2], parts_recv_sem.at[2], mz, mx, mate)

    mine = pl.ds(pl.multiple_of(16 * bank, 16), 16)

    def serve_rows():
        wait(parts.at[0], parts_recv_sem.at[2])
        low = half[0:8]
        for t in range(16):
            z, x = t // 4, t % 4
            a = parts[0, z, x].astype(jnp.float32)
            b = parts[1, z, x].astype(jnp.float32)
            block = jnp.concatenate(
                [
                    jnp.where(low, a, pltpu.roll(b, 64, 1)),
                    jnp.where(low, pltpu.roll(a, 64, 1), b),
                ],
                axis=0,
            )
            router[mine, 128 * t : 128 * t + 128] = block.astype(jnp.bfloat16)
        for i in range(1, 4):
            pltpu.make_async_remote_copy(
                src_ref=router.at[mine],
                dst_ref=router.at[mine],
                send_sem=row_send_sem,
                recv_sem=row_recv_sem,
                device_id={"bank": turn(bank, i)},
                device_id_type=MESH,
            ).start()

    def step(c, _):
        go_on(c)

        @pl.when(c < CHUNKS - AHEAD)
        def _():
            code_and_leave(c + AHEAD, 0)

        decode(c - 2)

        @pl.when(c == CHUNKS // 2)
        def _():
            serve_rows()

        return 0

    lax.fori_loop(2, CHUNKS, step, 0)
    decode(CHUNKS - 2)
    rest = pl.ds(0, 48)
    wait(router.at[rest], row_recv_sem)
    wait(router.at[rest], row_send_sem)
    wait(parts.at[0, 0, three], parts_send_sem.at[0])
    wait(parts.at[0, three], parts_send_sem.at[1])
    wait(parts.at[0], parts_send_sem.at[2])
    wait(sums_send.at[three], sums_send_sem)
    wait(sums_recv.at[pl.ds(0, 7)], sums_pass_sem)
    every = pl.ds(0, CHUNKS)
    both = pl.ds(0, 2)
    wait(send.at[both, every, three], send_sem)
    for h in range(2):
        wait(recv.at[h, CHUNKS - 1, pl.ds(0, 7)], recv_sem.at[h, CHUNKS - 1])
    wait(recv.at[both, every, pl.ds(0, 7)], pass_sem)


def hand_out(
    out, scale, router, recv, table,
    gate, up, down, sg, su, sd, served,
    last, sem,
):
    few = 4 * PER
    copies = []

    def copy(src, dst):
        copies.append(pltpu.make_async_copy(src, dst, sem.at[len(copies)]))
        copies[-1].start()

    for a, (big, small) in enumerate(((gate, sg), (up, su), (down, sd))):
        count = 16 - few * (a == 2)
        copy(out.at[pl.ds(16 * a, count)], big.at[pl.ds(0, count)])
        copy(scale.at[pl.ds(16 * a, 16)], small)
    copy(router, served)
    for h in range(2):

        def go(k, _):
            decode_pair(recv, table, last, CHUNKS - 1, h, k, h * PER + k)
            return 0

        lax.fori_loop(0, PER, go, 0)
        part = 2 * PER
        copy(last.at[pl.ds(part * h, part)], down.at[pl.ds(16 - few + part * h, part)])
    for c in copies:
        c.wait()


def body(gate, up, down, weight, gain):
    vmem = pl.BlockSpec(memory_space=pltpu.VMEM)
    hbm = pl.BlockSpec(memory_space=pltpu.HBM)
    f32, bf16 = jnp.float32, jnp.bfloat16
    dma = pltpu.SemaphoreType.DMA
    results = pl.pallas_call(
        exchange,
        name="exchange",
        out_shape=(
            pltpu.VMEM((48, 32, 2048), bf16),
            pltpu.VMEM((48, 32), f32),
            pltpu.VMEM((64, 2048), bf16),
            pltpu.VMEM((2, CHUNKS, 8, 4, ROWS, 128), bf16),
            pltpu.VMEM((64, 32, 128), f32),
        ),
        in_specs=[hbm, hbm, hbm, vmem, vmem],
        out_specs=(vmem,) * 5,
        scratch_shapes=[
            pltpu.VMEM((48, 64, 1024), f32),
            pltpu.VMEM((2, CHUNKS, 4, 8, ROWS, 128), bf16),
            pltpu.VMEM((2, CHUNKS, 4, 8, ROWS, 128), bf16),
            pltpu.VMEM((48, 1, 1024), f32),
            pltpu.VMEM((4, 8, 16, 128), f32),
            pltpu.VMEM((4, 8, 16, 128), f32),
            pltpu.VMEM((8, 4, 16, 128), f32),
            pltpu.VMEM((2, 4, 4, 8, 128), bf16),
            dma((12,)),
            dma,
            dma((2, CHUNKS)),
            dma,
            dma((2, CHUNKS)),
            dma,
            dma,
            dma,
            dma,
            dma((3,)),
            dma((3,)),
            dma,
            dma,
        ],
        compiler_params=pltpu.CompilerParams(
            collective_id=0, has_side_effects=True, vmem_limit_bytes=49 * 2**20
        ),
    )(gate, up, jnp.swapaxes(down, 1, 2), weight.T, gain.reshape(1, 64))
    half = jax.ShapeDtypeStruct((16, 32, 2048), bf16)
    few = jax.ShapeDtypeStruct((16, 32), f32)
    gate, up, down, sg, su, sd, served = pl.pallas_call(
        hand_out,
        name="hand_out",
        out_shape=(half, half, half, few, few, few, jax.ShapeDtypeStruct((64, 2048), bf16)),
        in_specs=[vmem] * 5,
        out_specs=(hbm,) * 7,
        scratch_shapes=[pltpu.VMEM((4 * PER, 32, 2048), bf16), dma((9,))],
        compiler_params=pltpu.CompilerParams(vmem_limit_bytes=16 * 2**20),
    )(*(pltpu.with_memory_space_constraint(a, pltpu.VMEM) for a in results))
    return (
        jnp.swapaxes(gate, 1, 2),
        jnp.swapaxes(up, 1, 2),
        down,
        sg,
        su,
        sd,
        served.T,
    )


def solution(mesh):
    return jax.shard_map(
        body,
        mesh=mesh,
        in_specs=(
            P("bank", "zero", None),
            P("bank", "zero", None),
            P("bank", None, "zero"),
            P("zero", "bank"),
            P("zero"),
        ),
        out_specs=(
            P("bank", None, "zero"),
            P("bank", None, "zero"),
            P("bank", "zero", None),
            P("bank", "zero"),
            P("bank", "zero"),
            P("bank", "zero"),
            P(),
        ),
        check_vma=False,
    )
```

```python
import jax
import jax.numpy as jnp
from jax import lax
from jax.experimental import pallas as pl
from jax.experimental.pallas import tpu as pltpu
from jax.sharding import PartitionSpec as P

MESH = pl.DeviceIdType.MESH
CHUNKS = 12
AHEAD = 4
LOAD = 4
PAIRS = 24
PER = PAIRS // CHUNKS // 2
ROWS = PER * 32
POWER = 20
UP = 2.0**6.25


def left_half():
    return lax.broadcasted_iota(jnp.int32, (32, 128), 1) < 64


def decode_pair(recv, table, out, totals, wide, c, h, k, place):
    half = left_half()
    p = (2 * c + h) * PER + k
    rows = pl.ds(pl.multiple_of(32 * k, 32), 32)
    f0 = table[2 * p]
    f1 = table[2 * p + 1]
    squares = [jnp.zeros((32, 128), jnp.float32)] * 2
    for t in range(16):
        z, x = t // 4, t % 4
        one, two = ((z, x), (x, z))[h]
        left, right = 8 * z + x, 8 * z + 4 + x
        columns = slice(128 * t, 128 * t + 128)
        a = recv[h, c, 2 * one, two, rows, :].astype(jnp.float32)
        b = recv[h, c, 2 * one + 1, two, rows, :].astype(jnp.float32)
        for e, f, u in (
            (0, f0, jnp.where(half, a, pltpu.roll(b, 64, 1))),
            (1, f1, jnp.where(half, pltpu.roll(a, 64, 1), b)),
        ):
            g = jnp.where(
                half,
                jnp.broadcast_to(f[:, left : left + 1], (32, 128)),
                jnp.broadcast_to(f[:, right : right + 1], (32, 128)),
            )
            m = jnp.exp(jnp.log(jnp.abs(u)) * (1.0 / POWER))
            v = jnp.where(u < 0.0, -m, m) * g
            wide[e, :, columns] = v
            squares[e] = squares[e] + v * v
    lane = lax.broadcasted_iota(jnp.int32, (32, 128), 1)
    for e in range(2):
        total = jnp.sum(squares[e], axis=1, keepdims=True)
        totals[...] = jnp.where(lane == 2 * p + e, total, totals[...])
        r = lax.rsqrt(total)
        for t in range(16):
            columns = slice(128 * t, 128 * t + 128)
            out[2 * place + e, :, columns] = (wide[e, :, columns] * r).astype(jnp.bfloat16)


def exchange(
    gate, up, down, weight, gain,
    out, totals, router, recv, table,
    xin, send, relay, sums, sums_send, sums_relay, sums_recv, parts, wide_rows,
    in_sem, send_sem, relay_sem, pass_sem, recv_sem,
    sums_send_sem, sums_relay_sem, sums_pass_sem, sums_recv_sem,
    parts_send_sem, parts_recv_sem, row_send_sem, row_recv_sem,
):
    me = lax.axis_index("zero")
    bank = lax.axis_index("bank")
    mz, mx, mc = lax.div(me, 8), lax.rem(lax.div(me, 2), 4), lax.rem(me, 2)
    mate = 1 - mc

    def turn(place, i):
        return lax.rem(place + i, 4)

    def device(z, x, c):
        return z * 8 + x * 2 + c

    def put(src, dst, sent, arrived, z, x, c):
        pltpu.make_async_remote_copy(
            src_ref=src,
            dst_ref=dst,
            send_sem=sent,
            recv_sem=arrived,
            device_id={"zero": device(z, x, c)},
            device_id_type=MESH,
        ).start()

    def wait(ref, sem):
        pltpu.make_async_copy(ref, ref, sem).wait()

    loads = [
        pltpu.make_async_copy(
            ref.at[pl.ds(k, LOAD)], xin.at[pl.ds(16 * a + k, LOAD)], in_sem.at[4 * a + k // LOAD]
        )
        for a, ref in enumerate((gate, up, down))
        for k in range(0, 16, LOAD)
    ]
    for copy in loads[:2]:
        copy.start()

    barrier = pltpu.get_barrier_semaphore()

    def greet(**where):
        pl.semaphore_signal(
            barrier, inc=1, device_id=where, device_id_type=MESH
        )

    greet(zero=device(mz, mx, mate))
    for i in (1, 3, 2):
        for c in range(2):
            greet(zero=device(turn(mz, i), mx, c))
            greet(zero=device(mz, turn(mx, i), c))
        greet(bank=turn(bank, i))

    part = (weight[...] * gain[...]).astype(jnp.bfloat16)
    parts[mc, mz, mx] = jnp.concatenate([part[0:8], part[8:16]], axis=1)

    def add_up(e, _):
        x = xin[e]
        norm = jnp.sqrt(jnp.sum(x * x, axis=0, keepdims=True))
        sums[e] = norm.astype(jnp.bfloat16).astype(jnp.float32)
        return 0

    def code_pair(c, h):
        def go(k, _):
            p = (2 * c + h) * PER + k
            rows = pl.ds(pl.multiple_of(32 * k, 32), 32)
            for b in range(8):
                columns = slice(128 * b, 128 * b + 128)
                halves = []
                for e in range(2):
                    s = sums[2 * p + e, :, columns]
                    r = jnp.where(s > 0.0, UP / s, 0.0)
                    halves.append(xin[2 * p + e, :, columns] * r)
                y = jnp.concatenate(halves, axis=0).T
                y2 = y * y
                y4 = y2 * y2
                y8 = y4 * y4
                y20 = y8 * y8 * y4
                u = jnp.where(y < 0.0, -y20, y20).astype(jnp.bfloat16)
                for q in range(4):
                    z, x, d = b // 2, b % 2 * 2 + q // 2, q % 2
                    first, second = ((x, z), (z, x))[h]
                    send[h, c, first, 2 * second + d, rows, :] = u[32 * q : 32 * q + 32]
            return 0

        return go

    def code(c):
        for h in range(2):
            lax.fori_loop(0, PER, code_pair(c, h), 0)

    def leave(c):
        for i in (1, 3, 2):
            x, z = turn(mx, i), turn(mz, i)
            put(send.at[0, c, x], relay.at[0, c, mx], send_sem, relay_sem.at[0, c], mz, x, mc)
            put(send.at[1, c, z], relay.at[1, c, mz], send_sem, relay_sem.at[1, c], z, mx, mc)
        relay[0, c, mx] = send[0, c, mx]
        relay[1, c, mz] = send[1, c, mz]

    four = pl.ds(0, 4)
    three = pl.ds(0, 3)

    def go_on(c):
        for h in range(2):
            wait(relay.at[h, c, three], relay_sem.at[h, c])
        at_z, at_x = 2 * mz + mc, 2 * mx + mc
        for i in (1, 3, 2):
            for d in range(2):
                x, z = turn(mx, i), turn(mz, i)
                put(relay.at[0, c, four, 2 * z + d], recv.at[0, c, at_z], pass_sem, recv_sem.at[0, c], z, mx, d)
                put(relay.at[1, c, four, 2 * x + d], recv.at[1, c, at_x], pass_sem, recv_sem.at[1, c], mz, x, d)
        put(relay.at[0, c, four, 2 * mz + mate], recv.at[0, c, at_z], pass_sem, recv_sem.at[0, c], mz, mx, mate)
        put(relay.at[1, c, four, 2 * mx + mate], recv.at[1, c, at_x], pass_sem, recv_sem.at[1, c], mz, mx, mate)
        recv[0, c, at_z] = relay[0, c, :, at_z]
        recv[1, c, at_x] = relay[1, c, :, at_x]

    loads[0].wait()
    for copy in loads[2:]:
        copy.start()
    lax.fori_loop(0, LOAD, add_up, 0)
    code(0)
    pl.semaphore_wait(barrier, 16)
    leave(0)
    loads[1].wait()
    lax.fori_loop(LOAD, 2 * LOAD, add_up, 0)
    code(1)
    leave(1)

    for i in range(2, 12):
        loads[i].wait()
        lax.fori_loop(LOAD * i, LOAD * i + LOAD, add_up, 0)

    pad = jnp.zeros((16, 128), jnp.float32)
    for b in range(8):
        s = sums[:, 0, 128 * b : 128 * b + 128]
        t = jnp.concatenate([s, pad, pltpu.roll(s, 112, 1), pad], axis=0).T
        for q in range(4):
            z, x, d = b // 2, b % 2 * 2 + q // 2, q % 2
            sums_send[x, 2 * z + d] = t[32 * q : 32 * q + 16].astype(jnp.bfloat16)
    for i in (1, 3, 2):
        x = turn(mx, i)
        put(sums_send.at[x], sums_relay.at[mx], sums_send_sem, sums_relay_sem, mz, x, mc)
        put(parts.at[mc, mz, mx], parts.at[mc, mz, mx], parts_send_sem.at[0], parts_recv_sem.at[0], mz, x, mc)
    sums_relay[mx] = sums_send[mx]

    def code_and_leave(c, _):
        code(c)
        leave(c)
        return 0

    lax.fori_loop(2, AHEAD, code_and_leave, 0)
    go_on(0)

    wait(sums_relay.at[three], sums_relay_sem)
    wait(parts.at[0, 0, three], parts_recv_sem.at[0])
    at_z = 2 * mz + mc
    for i in (1, 3, 2):
        z = turn(mz, i)
        for d in range(2):
            put(sums_relay.at[four, 2 * z + d], sums_recv.at[at_z], sums_pass_sem, sums_recv_sem, z, mx, d)
        put(parts.at[mc, mz], parts.at[mc, mz], parts_send_sem.at[1], parts_recv_sem.at[1], z, mx, mc)
    put(sums_relay.at[four, 2 * mz + mate], sums_recv.at[at_z], sums_pass_sem, sums_recv_sem, mz, mx, mate)
    sums_recv[at_z] = sums_relay[:, at_z]

    code_and_leave(AHEAD, 0)
    go_on(1)
    code_and_leave(AHEAD + 1, 0)

    wait(sums_recv.at[pl.ds(0, 7)], sums_recv_sem)
    wide = sums_recv[...].astype(jnp.float32).reshape(32, 16, 128)
    for n in range(16):
        rows = jnp.concatenate([wide[:, n, :], jnp.zeros((96, 128), jnp.float32)], axis=0).T
        table[:, n, :] = rows[0:64] * (1.0 / UP)
        table[:, n + 16, :] = rows[64:128] * (1.0 / UP)
    totals[...] = jnp.zeros_like(totals)

    half = left_half()

    def decode(c):
        for h in range(2):
            wait(recv.at[h, c, pl.ds(0, 7)], recv_sem.at[h, c])

            def go(k, _):
                decode_pair(recv, table, out, totals, wide_rows, c, h, k, (2 * c + h) * PER + k)
                return 0

            lax.fori_loop(0, PER, go, 0)

    wait(parts.at[0, three], parts_recv_sem.at[1])
    put(parts.at[mc], parts.at[mc], parts_send_sem.at[2], parts_recv_sem.at[2], mz, mx, mate)

    mine = pl.ds(pl.multiple_of(16 * bank, 16), 16)

    def serve_rows():
        wait(parts.at[0], parts_recv_sem.at[2])
        low = half[0:8]
        for t in range(16):
            z, x = t // 4, t % 4
            a = parts[0, z, x].astype(jnp.float32)
            b = parts[1, z, x].astype(jnp.float32)
            block = jnp.concatenate(
                [
                    jnp.where(low, a, pltpu.roll(b, 64, 1)),
                    jnp.where(low, pltpu.roll(a, 64, 1), b),
                ],
                axis=0,
            )
            router[mine, 128 * t : 128 * t + 128] = block.astype(jnp.bfloat16)
        for i in range(1, 4):
            pltpu.make_async_remote_copy(
                src_ref=router.at[mine],
                dst_ref=router.at[mine],
                send_sem=row_send_sem,
                recv_sem=row_recv_sem,
                device_id={"bank": turn(bank, i)},
                device_id_type=MESH,
            ).start()

    def step(c, _):
        go_on(c)

        @pl.when(c < CHUNKS - AHEAD)
        def _():
            code_and_leave(c + AHEAD, 0)

        decode(c - 2)

        @pl.when(c == CHUNKS // 2)
        def _():
            serve_rows()

        return 0

    lax.fori_loop(2, CHUNKS, step, 0)
    decode(CHUNKS - 2)
    rest = pl.ds(0, 48)
    wait(router.at[rest], row_recv_sem)
    wait(router.at[rest], row_send_sem)
    wait(parts.at[0, 0, three], parts_send_sem.at[0])
    wait(parts.at[0, three], parts_send_sem.at[1])
    wait(parts.at[0], parts_send_sem.at[2])
    wait(sums_send.at[three], sums_send_sem)
    wait(sums_recv.at[pl.ds(0, 7)], sums_pass_sem)
    every = pl.ds(0, CHUNKS)
    both = pl.ds(0, 2)
    wait(send.at[both, every, three], send_sem)
    for h in range(2):
        wait(recv.at[h, CHUNKS - 1, pl.ds(0, 7)], recv_sem.at[h, CHUNKS - 1])
    wait(recv.at[both, every, pl.ds(0, 7)], pass_sem)


def hand_out(
    out, begun, router, recv, table,
    gate, up, down, sg, su, sd, served,
    last, totals, scale, wide_rows, sem,
):
    few = 4 * PER
    copies = []

    def copy(src, dst):
        copies.append(pltpu.make_async_copy(src, dst, sem.at[len(copies)]))
        copies[-1].start()

    for a, big in enumerate((gate, up, down)):
        count = 16 - few * (a == 2)
        copy(out.at[pl.ds(16 * a, count)], big.at[pl.ds(0, count)])
    copy(router, served)
    totals[...] = begun[...]
    for h in range(2):

        def go(k, _):
            decode_pair(recv, table, last, totals, wide_rows, CHUNKS - 1, h, k, h * PER + k)
            return 0

        lax.fori_loop(0, PER, go, 0)
        part = 2 * PER
        copy(last.at[pl.ds(part * h, part)], down.at[pl.ds(16 - few + part * h, part)])
    turned = jnp.concatenate([totals[...], jnp.zeros((96, 128), jnp.float32)], axis=0).T
    scale[...] = jnp.sqrt(turned[0:48, 0:32])
    for a, small in enumerate((sg, su, sd)):
        copy(scale.at[pl.ds(16 * a, 16)], small)
    for c in copies:
        c.wait()


def body(gate, up, down, weight, gain):
    vmem = pl.BlockSpec(memory_space=pltpu.VMEM)
    hbm = pl.BlockSpec(memory_space=pltpu.HBM)
    f32, bf16 = jnp.float32, jnp.bfloat16
    dma = pltpu.SemaphoreType.DMA
    results = pl.pallas_call(
        exchange,
        name="exchange",
        out_shape=(
            pltpu.VMEM((48, 32, 2048), bf16),
            pltpu.VMEM((32, 128), f32),
            pltpu.VMEM((64, 2048), bf16),
            pltpu.VMEM((2, CHUNKS, 8, 4, ROWS, 128), bf16),
            pltpu.VMEM((64, 32, 128), f32),
        ),
        in_specs=[hbm, hbm, hbm, vmem, vmem],
        out_specs=(vmem,) * 5,
        scratch_shapes=[
            pltpu.VMEM((48, 64, 1024), f32),
            pltpu.VMEM((2, CHUNKS, 4, 8, ROWS, 128), bf16),
            pltpu.VMEM((2, CHUNKS, 4, 8, ROWS, 128), bf16),
            pltpu.VMEM((48, 1, 1024), f32),
            pltpu.VMEM((4, 8, 16, 128), bf16),
            pltpu.VMEM((4, 8, 16, 128), bf16),
            pltpu.VMEM((8, 4, 16, 128), bf16),
            pltpu.VMEM((2, 4, 4, 8, 128), bf16),
            pltpu.VMEM((2, 32, 2048), f32),
            dma((12,)),
            dma,
            dma((2, CHUNKS)),
            dma,
            dma((2, CHUNKS)),
            dma,
            dma,
            dma,
            dma,
            dma((3,)),
            dma((3,)),
            dma,
            dma,
        ],
        compiler_params=pltpu.CompilerParams(
            collective_id=0, has_side_effects=True, vmem_limit_bytes=49 * 2**20
        ),
    )(gate, up, jnp.swapaxes(down, 1, 2), weight.T, gain.reshape(1, 64))
    half = jax.ShapeDtypeStruct((16, 32, 2048), bf16)
    few = jax.ShapeDtypeStruct((16, 32), f32)
    gate, up, down, sg, su, sd, served = pl.pallas_call(
        hand_out,
        name="hand_out",
        out_shape=(half, half, half, few, few, few, jax.ShapeDtypeStruct((64, 2048), bf16)),
        in_specs=[vmem] * 5,
        out_specs=(hbm,) * 7,
        scratch_shapes=[
            pltpu.VMEM((4 * PER, 32, 2048), bf16),
            pltpu.VMEM((32, 128), f32),
            pltpu.VMEM((48, 32), f32),
            pltpu.VMEM((2, 32, 2048), f32),
            dma((9,)),
        ],
        compiler_params=pltpu.CompilerParams(vmem_limit_bytes=16 * 2**20),
    )(*(pltpu.with_memory_space_constraint(a, pltpu.VMEM) for a in results))
    return (
        jnp.swapaxes(gate, 1, 2),
        jnp.swapaxes(up, 1, 2),
        down,
        sg,
        su,
        sd,
        served.T,
    )


def solution(mesh):
    return jax.shard_map(
        body,
        mesh=mesh,
        in_specs=(
            P("bank", "zero", None),
            P("bank", "zero", None),
            P("bank", None, "zero"),
            P("zero", "bank"),
            P("zero"),
        ),
        out_specs=(
            P("bank", None, "zero"),
            P("bank", None, "zero"),
            P("bank", "zero", None),
            P("bank", "zero"),
            P("bank", "zero"),
            P("bank", "zero"),
            P(),
        ),
        check_vma=False,
    )
```

```python
import jax
import jax.numpy as jnp
from jax import lax
from jax.experimental import pallas as pl
from jax.experimental.pallas import tpu as pltpu
from jax.sharding import PartitionSpec as P

MESH = pl.DeviceIdType.MESH
CHUNKS = 12
AHEAD = 4
PAIRS = 24
POWER = 20
UP = 2.0**6.25


def turned(h, a, b):
    return a + h * (b - a), b + h * (a - b)


def left_half():
    return lax.broadcasted_iota(jnp.int32, (32, 128), 1) < 64


def decode_pair(recv, table, out, totals, wide, p, place):
    half = left_half()
    h = lax.rem(p, 2)
    f0 = table[2 * p]
    f1 = table[2 * p + 1]
    squares = [jnp.zeros((32, 128), jnp.float32)] * 2
    for t in range(16):
        z, x = t // 4, t % 4
        one, two = turned(h, z, x)
        left, right = 8 * z + x, 8 * z + 4 + x
        columns = slice(128 * t, 128 * t + 128)
        a = recv[p, 2 * one, two].astype(jnp.float32)
        b = recv[p, 2 * one + 1, two].astype(jnp.float32)
        for e, f, u in (
            (0, f0, jnp.where(half, a, pltpu.roll(b, 64, 1))),
            (1, f1, jnp.where(half, pltpu.roll(a, 64, 1), b)),
        ):
            g = jnp.where(
                half,
                jnp.broadcast_to(f[:, left : left + 1], (32, 128)),
                jnp.broadcast_to(f[:, right : right + 1], (32, 128)),
            )
            m = jnp.exp(jnp.log(jnp.abs(u)) * (1.0 / POWER))
            v = jnp.where(u < 0.0, -m, m) * g
            wide[e, :, columns] = v
            squares[e] = squares[e] + v * v
    lane = lax.broadcasted_iota(jnp.int32, (32, 128), 1)
    for e in range(2):
        total = jnp.sum(squares[e], axis=1, keepdims=True)
        totals[...] = jnp.where(lane == 2 * p + e, total, totals[...])
        r = lax.rsqrt(total)
        for t in range(16):
            columns = slice(128 * t, 128 * t + 128)
            out[2 * place + e, :, columns] = (wide[e, :, columns] * r).astype(jnp.bfloat16)


def exchange(
    gate, up, down, weight, gain,
    out, totals, router, recv, table,
    xin, send, relay, sums, sums_send, sums_relay, sums_recv, parts, wide_rows,
    in_sem, send_sem, relay_sem, pass_sem, recv_sem,
    sums_send_sem, sums_relay_sem, sums_pass_sem, sums_recv_sem,
    parts_send_sem, parts_recv_sem, row_send_sem, row_recv_sem,
):
    me = lax.axis_index("zero")
    bank = lax.axis_index("bank")
    mz, mx, mc = lax.div(me, 8), lax.rem(lax.div(me, 2), 4), lax.rem(me, 2)
    mate = 1 - mc

    def turn(place, i):
        return lax.rem(place + i, 4)

    def device(z, x, c):
        return z * 8 + x * 2 + c

    def put(src, dst, sent, arrived, z, x, c):
        pltpu.make_async_remote_copy(
            src_ref=src,
            dst_ref=dst,
            send_sem=sent,
            recv_sem=arrived,
            device_id={"zero": device(z, x, c)},
            device_id_type=MESH,
        ).start()

    def wait(ref, sem):
        pltpu.make_async_copy(ref, ref, sem).wait()

    loads = [
        pltpu.make_async_copy(
            ref.at[pl.ds(k, count)], xin.at[pl.ds(16 * a + k, count)], in_sem.at[i]
        )
        for i, (a, ref, k, count) in enumerate(((0, gate, 0, 4), (0, gate, 4, 4), (0, gate, 8, 8), (1, up, 0, 16), (2, down, 0, 16)))
    ]
    for copy in loads[:2]:
        copy.start()

    barrier = pltpu.get_barrier_semaphore()

    def greet(**where):
        pl.semaphore_signal(
            barrier, inc=1, device_id=where, device_id_type=MESH
        )

    greet(zero=device(mz, mx, mate))
    for i in (1, 3, 2):
        for c in range(2):
            greet(zero=device(turn(mz, i), mx, c))
            greet(zero=device(mz, turn(mx, i), c))
        greet(bank=turn(bank, i))

    part = (weight[...] * gain[...]).astype(jnp.bfloat16)
    parts[mc, mz, mx] = jnp.concatenate([part[0:8], part[8:16]], axis=1)

    def add_up(e, _):
        x = xin[e]
        norm = jnp.sqrt(jnp.sum(x * x, axis=0, keepdims=True))
        sums[e] = norm.astype(jnp.bfloat16).astype(jnp.float32)
        return 0

    def code(p):
        h = lax.rem(p, 2)
        for b in range(8):
            columns = slice(128 * b, 128 * b + 128)
            halves = []
            for e in range(2):
                s = sums[2 * p + e, :, columns]
                r = jnp.where(s > 0.0, UP / s, 0.0)
                halves.append(xin[2 * p + e, :, columns] * r)
            y = jnp.concatenate(halves, axis=0).T
            y2 = y * y
            y4 = y2 * y2
            y8 = y4 * y4
            y20 = y8 * y8 * y4
            u = jnp.where(y < 0.0, -y20, y20).astype(jnp.bfloat16)
            for q in range(4):
                z, x, d = b // 2, b % 2 * 2 + q // 2, q % 2
                first, second = turned(h, x, z)
                send[p, first, 2 * second + d] = u[32 * q : 32 * q + 32]

    def leave(p):
        h = lax.rem(p, 2)
        mine, other = turned(h, mx, mz)
        for i in (2, 1, 3):
            to = turn(mine, i)
            x, z = turned(h, to, other)
            put(send.at[p, to], relay.at[p, mine], send_sem, relay_sem.at[p], z, x, mc)
        relay[p, mine] = send[p, mine]

    four = pl.ds(0, 4)
    three = pl.ds(0, 3)

    def go_on(p):
        h = lax.rem(p, 2)
        wait(relay.at[p, three], relay_sem.at[p])
        mine, other = turned(h, mz, mx)
        slot = 2 * mine + mc
        put(relay.at[p, four, 2 * mine + mate], recv.at[p, slot], pass_sem, recv_sem.at[p], mz, mx, mate)
        for i in (2, 1, 3):
            to = turn(mine, i)
            z, x = turned(h, to, other)
            for d in range(2):
                put(relay.at[p, four, 2 * to + d], recv.at[p, slot], pass_sem, recv_sem.at[p], z, x, d)
        recv[p, slot] = relay[p, :, slot]

    def each(act, c):
        def go(p, _):
            act(p)
            return 0

        lax.fori_loop(2 * c, 2 * c + 2, go, 0)

    def code_and_leave(p):
        code(p)
        leave(p)

    loads[0].wait()
    lax.fori_loop(0, 4, add_up, 0)

    each(code, 0)
    pl.semaphore_wait(barrier, 16)
    each(leave, 0)
    for copy in loads[2:]:
        copy.start()
    loads[1].wait()
    lax.fori_loop(4, 8, add_up, 0)
    each(code_and_leave, 1)
    for copy, low, high in zip(loads[2:], (8, 16, 32), (16, 32, 48)):
        copy.wait()
        lax.fori_loop(low, high, add_up, 0)

    pad = jnp.zeros((16, 128), jnp.float32)
    for b in range(8):
        s = sums[:, 0, 128 * b : 128 * b + 128]
        t = jnp.concatenate([s, pad, pltpu.roll(s, 112, 1), pad], axis=0).T
        for q in range(4):
            z, x, d = b // 2, b % 2 * 2 + q // 2, q % 2
            sums_send[x, 2 * z + d] = t[32 * q : 32 * q + 16].astype(jnp.bfloat16)
    for i in (1, 3, 2):
        x = turn(mx, i)
        put(sums_send.at[x], sums_relay.at[mx], sums_send_sem, sums_relay_sem, mz, x, mc)
        put(parts.at[mc, mz, mx], parts.at[mc, mz, mx], parts_send_sem.at[0], parts_recv_sem.at[0], mz, x, mc)
    sums_relay[mx] = sums_send[mx]

    for c in range(2, AHEAD):
        each(code_and_leave, c)
    each(go_on, 0)

    wait(sums_relay.at[three], sums_relay_sem)
    wait(parts.at[0, 0, three], parts_recv_sem.at[0])
    at_z = 2 * mz + mc
    for i in (1, 3, 2):
        z = turn(mz, i)
        for d in range(2):
            put(sums_relay.at[four, 2 * z + d], sums_recv.at[at_z], sums_pass_sem, sums_recv_sem, z, mx, d)
        put(parts.at[mc, mz], parts.at[mc, mz], parts_send_sem.at[1], parts_recv_sem.at[1], z, mx, mc)
    put(sums_relay.at[four, 2 * mz + mate], sums_recv.at[at_z], sums_pass_sem, sums_recv_sem, mz, mx, mate)
    sums_recv[at_z] = sums_relay[:, at_z]

    each(code_and_leave, AHEAD)
    each(go_on, 1)
    each(code_and_leave, AHEAD + 1)

    wait(sums_recv.at[pl.ds(0, 7)], sums_recv_sem)
    wide = sums_recv[...].astype(jnp.float32).reshape(32, 16, 128)
    for n in range(16):
        rows = jnp.concatenate([wide[:, n, :], jnp.zeros((96, 128), jnp.float32)], axis=0).T
        table[:, n, :] = rows[0:64] * (1.0 / UP)
        table[:, n + 16, :] = rows[64:128] * (1.0 / UP)
    totals[...] = jnp.zeros_like(totals)

    half = left_half()

    def decode(p):
        wait(recv.at[p, pl.ds(0, 7)], recv_sem.at[p])
        decode_pair(recv, table, out, totals, wide_rows, p, p)

    wait(parts.at[0, three], parts_recv_sem.at[1])
    put(parts.at[mc], parts.at[mc], parts_send_sem.at[2], parts_recv_sem.at[2], mz, mx, mate)

    mine = pl.ds(pl.multiple_of(16 * bank, 16), 16)

    def serve_rows():
        wait(parts.at[0], parts_recv_sem.at[2])
        low = half[0:8]
        for t in range(16):
            z, x = t // 4, t % 4
            a = parts[0, z, x].astype(jnp.float32)
            b = parts[1, z, x].astype(jnp.float32)
            block = jnp.concatenate(
                [
                    jnp.where(low, a, pltpu.roll(b, 64, 1)),
                    jnp.where(low, pltpu.roll(a, 64, 1), b),
                ],
                axis=0,
            )
            router[mine, 128 * t : 128 * t + 128] = block.astype(jnp.bfloat16)
        for i in range(1, 4):
            pltpu.make_async_remote_copy(
                src_ref=router.at[mine],
                dst_ref=router.at[mine],
                send_sem=row_send_sem,
                recv_sem=row_recv_sem,
                device_id={"bank": turn(bank, i)},
                device_id_type=MESH,
            ).start()

    def step(c, _):
        each(go_on, c)

        @pl.when(c < CHUNKS - AHEAD)
        def _():
            each(code_and_leave, c + AHEAD)

        each(decode, c - 2)

        @pl.when(c == CHUNKS // 2)
        def _():
            serve_rows()

        return 0

    lax.fori_loop(2, CHUNKS, step, 0)
    each(decode, CHUNKS - 2)
    rest = pl.ds(0, 48)
    wait(router.at[rest], row_recv_sem)
    wait(router.at[rest], row_send_sem)
    wait(parts.at[0, 0, three], parts_send_sem.at[0])
    wait(parts.at[0, three], parts_send_sem.at[1])
    wait(parts.at[0], parts_send_sem.at[2])
    wait(sums_send.at[three], sums_send_sem)
    wait(sums_recv.at[pl.ds(0, 7)], sums_pass_sem)
    every = pl.ds(0, PAIRS)
    wait(send.at[every, three], send_sem)
    for p in range(PAIRS - 2, PAIRS):
        wait(recv.at[p, pl.ds(0, 7)], recv_sem.at[p])
    wait(recv.at[every, pl.ds(0, 7)], pass_sem)


def hand_out(
    out, begun, router, recv, table,
    gate, up, down, sg, su, sd, served,
    last, totals, scale, wide_rows, sem,
):
    few = 4
    copies = []

    def copy(src, dst):
        copies.append(pltpu.make_async_copy(src, dst, sem.at[len(copies)]))
        copies[-1].start()

    for a, big in enumerate((gate, up, down)):
        count = 16 - few * (a == 2)
        copy(out.at[pl.ds(16 * a, count)], big.at[pl.ds(0, count)])
    copy(router, served)
    totals[...] = begun[...]

    def go(i, _):
        decode_pair(recv, table, last, totals, wide_rows, PAIRS - 2 + i, i)
        return 0

    lax.fori_loop(0, 2, go, 0)
    copy(last, down.at[pl.ds(16 - few, few)])
    across = jnp.concatenate([totals[...], jnp.zeros((96, 128), jnp.float32)], axis=0).T
    scale[...] = jnp.sqrt(across[0:48, 0:32])
    for a, small in enumerate((sg, su, sd)):
        copy(scale.at[pl.ds(16 * a, 16)], small)
    for c in copies:
        c.wait()


def body(gate, up, down, weight, gain):
    vmem = pl.BlockSpec(memory_space=pltpu.VMEM)
    hbm = pl.BlockSpec(memory_space=pltpu.HBM)
    f32, bf16 = jnp.float32, jnp.bfloat16
    dma = pltpu.SemaphoreType.DMA
    results = pl.pallas_call(
        exchange,
        name="exchange",
        out_shape=(
            pltpu.VMEM((48, 32, 2048), bf16),
            pltpu.VMEM((32, 128), f32),
            pltpu.VMEM((64, 2048), bf16),
            pltpu.VMEM((PAIRS, 8, 4, 32, 128), bf16),
            pltpu.VMEM((64, 32, 128), f32),
        ),
        in_specs=[hbm, hbm, hbm, vmem, vmem],
        out_specs=(vmem,) * 5,
        scratch_shapes=[
            pltpu.VMEM((48, 64, 1024), f32),
            pltpu.VMEM((PAIRS, 4, 8, 32, 128), bf16),
            pltpu.VMEM((PAIRS, 4, 8, 32, 128), bf16),
            pltpu.VMEM((48, 1, 1024), f32),
            pltpu.VMEM((4, 8, 16, 128), bf16),
            pltpu.VMEM((4, 8, 16, 128), bf16),
            pltpu.VMEM((8, 4, 16, 128), bf16),
            pltpu.VMEM((2, 4, 4, 8, 128), bf16),
            pltpu.VMEM((2, 32, 2048), f32),
            dma((5,)),
            dma,
            dma((PAIRS,)),
            dma,
            dma((PAIRS,)),
            dma,
            dma,
            dma,
            dma,
            dma((3,)),
            dma((3,)),
            dma,
            dma,
        ],
        compiler_params=pltpu.CompilerParams(
            collective_id=0, has_side_effects=True, vmem_limit_bytes=49 * 2**20
        ),
    )(gate, up, jnp.swapaxes(down, 1, 2), weight.T, gain.reshape(1, 64))
    half = jax.ShapeDtypeStruct((16, 32, 2048), bf16)
    few = jax.ShapeDtypeStruct((16, 32), f32)
    gate, up, down, sg, su, sd, served = pl.pallas_call(
        hand_out,
        name="hand_out",
        out_shape=(half, half, half, few, few, few, jax.ShapeDtypeStruct((64, 2048), bf16)),
        in_specs=[vmem] * 5,
        out_specs=(hbm,) * 7,
        scratch_shapes=[
            pltpu.VMEM((4, 32, 2048), bf16),
            pltpu.VMEM((32, 128), f32),
            pltpu.VMEM((48, 32), f32),
            pltpu.VMEM((2, 32, 2048), f32),
            dma((8,)),
        ],
        compiler_params=pltpu.CompilerParams(vmem_limit_bytes=16 * 2**20),
    )(*(pltpu.with_memory_space_constraint(a, pltpu.VMEM) for a in results))
    return (
        jnp.swapaxes(gate, 1, 2),
        jnp.swapaxes(up, 1, 2),
        down,
        sg,
        su,
        sd,
        served.T,
    )


def solution(mesh):
    return jax.shard_map(
        body,
        mesh=mesh,
        in_specs=(
            P("bank", "zero", None),
            P("bank", "zero", None),
            P("bank", None, "zero"),
            P("zero", "bank"),
            P("zero"),
        ),
        out_specs=(
            P("bank", None, "zero"),
            P("bank", None, "zero"),
            P("bank", "zero", None),
            P("bank", "zero"),
            P("bank", "zero"),
            P("bank", "zero"),
            P(),
        ),
        check_vma=False,
    )
```

```python
import jax
import jax.numpy as jnp
from jax import lax
from jax.experimental import pallas as pl
from jax.experimental.pallas import tpu as pltpu
from jax.sharding import PartitionSpec as P

MESH = pl.DeviceIdType.MESH
CHUNKS = 12
OWN, SHARED = 16, 16
LAG = 4
AHEAD = 4
PAIRS = 24
POWER = 20
UP = 2.0**6.25


def turned(h, a, b):
    return a + h * (b - a), b + h * (a - b)


def left_half():
    return lax.broadcasted_iota(jnp.int32, (32, 128), 1) < 64


def decode_pair(recv, table, out, totals, wide, p, place):
    half = left_half()
    h = lax.rem(p, 2)
    f0 = table[2 * p]
    f1 = table[2 * p + 1]
    squares = [jnp.zeros((32, 128), jnp.float32)] * 2
    for t in range(16):
        z, x = t // 4, t % 4
        one, two = turned(h, z, x)
        left, right = 8 * z + x, 8 * z + 4 + x
        columns = slice(128 * t, 128 * t + 128)
        a = recv[p, 2 * one, two].astype(jnp.float32)
        b = recv[p, 2 * one + 1, two].astype(jnp.float32)
        for e, f, u in (
            (0, f0, jnp.where(half, a, pltpu.roll(b, 64, 1))),
            (1, f1, jnp.where(half, pltpu.roll(a, 64, 1), b)),
        ):
            g = jnp.where(
                half,
                jnp.broadcast_to(f[:, left : left + 1], (32, 128)),
                jnp.broadcast_to(f[:, right : right + 1], (32, 128)),
            )
            m = jnp.exp(jnp.log(jnp.abs(u)) * (1.0 / POWER))
            v = jnp.where(u < 0.0, -m, m) * g
            wide[e, :, columns] = v
            squares[e] = squares[e] + v * v
    lane = lax.broadcasted_iota(jnp.int32, (32, 128), 1)
    for e in range(2):
        total = jnp.sum(squares[e], axis=1, keepdims=True)
        totals[...] = jnp.where(lane == 2 * p + e, total, totals[...])
        r = lax.rsqrt(total)
        for t in range(16):
            columns = slice(128 * t, 128 * t + 128)
            out[2 * place + e, :, columns] = (wide[e, :, columns] * r).astype(jnp.bfloat16)


def exchange(
    gate, up, down, weight, gain,
    out, totals, router, recv, table,
    xin, send, relay, squares, sums, sums_send, sums_relay, sums_recv, parts, wide_rows,
    in_sem, send_sem, relay_sem, pass_sem, recv_sem,
    sums_send_sem, sums_relay_sem, sums_pass_sem, sums_recv_sem,
    parts_send_sem, parts_recv_sem, row_send_sem, row_recv_sem,
    mate_send_sem, mate_recv_sem,
):
    me = lax.axis_index("zero")
    bank = lax.axis_index("bank")
    mz, mx, mc = lax.div(me, 8), lax.rem(lax.div(me, 2), 4), lax.rem(me, 2)
    mate = 1 - mc

    def turn(place, i):
        return lax.rem(place + i, 4)

    def device(z, x, c):
        return z * 8 + x * 2 + c

    def put(src, dst, sent, arrived, z, x, c):
        pltpu.make_async_remote_copy(
            src_ref=src,
            dst_ref=dst,
            send_sem=sent,
            recv_sem=arrived,
            device_id={"zero": device(z, x, c)},
            device_id_type=MESH,
        ).start()

    def wait(ref, sem):
        pltpu.make_async_copy(ref, ref, sem).wait()

    loads = [
        pltpu.make_async_copy(
            ref.at[pl.ds(k, count)], xin.at[pl.ds(16 * a + k, count)], in_sem.at[i]
        )
        for i, (a, ref, k, count) in enumerate(((0, gate, 0, 4), (0, gate, 4, 4), (0, gate, 8, 8), (1, up, 0, 16), (2, down, 0, 16)))
    ]
    for copy in loads[:2]:
        copy.start()

    barrier = pltpu.get_barrier_semaphore()

    def greet(**where):
        pl.semaphore_signal(
            barrier, inc=1, device_id=where, device_id_type=MESH
        )

    greet(zero=device(mz, mx, mate))
    for i in (1, 3, 2):
        for c in range(2):
            greet(zero=device(turn(mz, i), mx, c))
            greet(zero=device(mz, turn(mx, i), c))
        greet(bank=turn(bank, i))

    part = (weight[...] * gain[...]).astype(jnp.bfloat16)
    parts[mc, mz, mx] = jnp.concatenate([part[0:8], part[8:16]], axis=1)

    def add_up(e, _):
        x = xin[e]
        squares[0, e] = jnp.sum(x * x, axis=0, keepdims=True)
        return 0

    def own_norm(e, _):
        sums[e] = jnp.sqrt(squares[0, e]).astype(jnp.bfloat16).astype(jnp.float32)
        return 0

    def chip_norm(e, _):
        norm = jnp.sqrt(squares[0, e] + squares[1, e])
        sums[e] = norm.astype(jnp.bfloat16).astype(jnp.float32)
        return 0

    def code(p):
        h = lax.rem(p, 2)
        for b in range(8):
            columns = slice(128 * b, 128 * b + 128)
            halves = []
            for e in range(2):
                s = sums[2 * p + e, :, columns]
                r = jnp.where(s > 0.0, UP / s, 0.0)
                halves.append(xin[2 * p + e, :, columns] * r)
            y = jnp.concatenate(halves, axis=0).T
            y2 = y * y
            y4 = y2 * y2
            y8 = y4 * y4
            y20 = y8 * y8 * y4
            u = jnp.where(y < 0.0, -y20, y20).astype(jnp.bfloat16)
            for q in range(4):
                z, x, d = b // 2, b % 2 * 2 + q // 2, q % 2
                first, second = turned(h, x, z)
                send[p, first, 2 * second + d] = u[32 * q : 32 * q + 32]

    def leave(p):
        h = lax.rem(p, 2)
        mine, other = turned(h, mx, mz)
        for i in (2, 1, 3):
            to = turn(mine, i)
            x, z = turned(h, to, other)
            put(send.at[p, to], relay.at[p, mine], send_sem, relay_sem.at[p], z, x, mc)
        relay[p, mine] = send[p, mine]

    four = pl.ds(0, 4)
    three = pl.ds(0, 3)

    def go_on(p):
        h = lax.rem(p, 2)
        wait(relay.at[p, three], relay_sem.at[p])
        mine, other = turned(h, mz, mx)
        slot = 2 * mine + mc
        put(relay.at[p, four, 2 * mine + mate], recv.at[p, slot], pass_sem, recv_sem.at[p], mz, mx, mate)
        for i in (2, 1, 3):
            to = turn(mine, i)
            z, x = turned(h, to, other)
            for d in range(2):
                put(relay.at[p, four, 2 * to + d], recv.at[p, slot], pass_sem, recv_sem.at[p], z, x, d)
        recv[p, slot] = relay[p, :, slot]

    def each(act, c):
        def go(p, _):
            act(p)
            return 0

        lax.fori_loop(2 * c, 2 * c + 2, go, 0)

    def code_and_leave(p):
        code(p)
        leave(p)

    loads[0].wait()
    lax.fori_loop(0, 4, add_up, 0)
    lax.fori_loop(0, 4, own_norm, 0)
    each(code, 0)
    pl.semaphore_wait(barrier, 16)
    each(leave, 0)
    for copy in loads[2:]:
        copy.start()
    loads[1].wait()
    lax.fori_loop(4, 8, add_up, 0)
    lax.fori_loop(4, 8, own_norm, 0)
    each(code_and_leave, 1)
    loads[2].wait()
    lax.fori_loop(8, OWN, add_up, 0)
    lax.fori_loop(8, OWN, own_norm, 0)
    each(code_and_leave, 2)
    each(code_and_leave, 3)

    for copy, low, high in zip(loads[3:], (16, 32), (32, 48)):
        copy.wait()
        lax.fori_loop(low, high, add_up, 0)
    rest = pl.ds(OWN, 48 - OWN)
    put(squares.at[0, rest], squares.at[1, rest], mate_send_sem, mate_recv_sem, mz, mx, mate)
    each(go_on, 0)
    wait(squares.at[1, rest], mate_recv_sem)
    lax.fori_loop(OWN, 48, chip_norm, 0)

    for b in range(8):
        columns = slice(128 * b, 128 * b + 128)
        s = jnp.concatenate(
            [
                sums[0:OWN, 0, columns],
                sums[pl.ds(OWN + SHARED * mc, SHARED), 0, columns],
            ],
            axis=0,
        )
        t = jnp.concatenate(
            [s] + [pltpu.roll(s, 128 - 8 * g, 1) for g in range(1, 4)], axis=0
        ).T
        for q in range(4):
            z, x, d = b // 2, b % 2 * 2 + q // 2, q % 2
            sums_send[x, 2 * z + d] = t[32 * q : 32 * q + 8].astype(jnp.bfloat16)
    for i in (1, 3, 2):
        x = turn(mx, i)
        put(sums_send.at[x], sums_relay.at[mx], sums_send_sem, sums_relay_sem, mz, x, mc)
        put(parts.at[mc, mz, mx], parts.at[mc, mz, mx], parts_send_sem.at[0], parts_recv_sem.at[0], mz, x, mc)
    sums_relay[mx] = sums_send[mx]

    each(code_and_leave, AHEAD)
    each(go_on, 1)
    each(code_and_leave, AHEAD + 1)

    wait(sums_relay.at[three], sums_relay_sem)
    wait(parts.at[0, 0, three], parts_recv_sem.at[0])
    at_z = 2 * mz + mc
    for i in (1, 3, 2):
        z = turn(mz, i)
        for d in range(2):
            put(sums_relay.at[four, 2 * z + d], sums_recv.at[at_z], sums_pass_sem, sums_recv_sem, z, mx, d)
        put(parts.at[mc, mz], parts.at[mc, mz], parts_send_sem.at[1], parts_recv_sem.at[1], z, mx, mc)
    put(sums_relay.at[four, 2 * mz + mate], sums_recv.at[at_z], sums_pass_sem, sums_recv_sem, mz, mx, mate)
    sums_recv[at_z] = sums_relay[:, at_z]

    for c in range(2, LAG):
        each(go_on, c)
        each(code_and_leave, AHEAD + c)

    wait(sums_recv.at[pl.ds(0, 7)], sums_recv_sem)
    wide = sums_recv[...].astype(jnp.float32).reshape(32, 8, 128)
    core = lax.rem(lax.div(lax.broadcasted_iota(jnp.int32, (128, 128), 1), 4), 2)
    for n in range(8):
        rows = jnp.concatenate([wide[:, n, :], jnp.zeros((96, 128), jnp.float32)], axis=0).T
        rows = rows * (1.0 / UP)
        low = jnp.where(core == 0, rows, pltpu.roll(rows, 4, 1))
        high = jnp.where(core == 1, rows, pltpu.roll(rows, 124, 1))
        for g in range(4):
            place = n + 8 * g
            own, chip = 32 * g, 32 * g + OWN
            table[0:OWN, place, :] = rows[own:chip]
            table[OWN : OWN + SHARED, place, :] = low[chip : chip + SHARED]
            table[OWN + SHARED : 48, place, :] = high[chip : chip + SHARED]
    totals[...] = jnp.zeros_like(totals)

    half = left_half()

    def decode(p):
        wait(recv.at[p, pl.ds(0, 7)], recv_sem.at[p])
        decode_pair(recv, table, out, totals, wide_rows, p, p)

    wait(parts.at[0, three], parts_recv_sem.at[1])
    put(parts.at[mc], parts.at[mc], parts_send_sem.at[2], parts_recv_sem.at[2], mz, mx, mate)

    mine = pl.ds(pl.multiple_of(16 * bank, 16), 16)

    def serve_rows():
        wait(parts.at[0], parts_recv_sem.at[2])
        low = half[0:8]
        for t in range(16):
            z, x = t // 4, t % 4
            a = parts[0, z, x].astype(jnp.float32)
            b = parts[1, z, x].astype(jnp.float32)
            block = jnp.concatenate(
                [
                    jnp.where(low, a, pltpu.roll(b, 64, 1)),
                    jnp.where(low, pltpu.roll(a, 64, 1), b),
                ],
                axis=0,
            )
            router[mine, 128 * t : 128 * t + 128] = block.astype(jnp.bfloat16)
        for i in range(1, 4):
            pltpu.make_async_remote_copy(
                src_ref=router.at[mine],
                dst_ref=router.at[mine],
                send_sem=row_send_sem,
                recv_sem=row_recv_sem,
                device_id={"bank": turn(bank, i)},
                device_id_type=MESH,
            ).start()

    def step(c, _):
        each(go_on, c)

        @pl.when(c < CHUNKS - AHEAD)
        def _():
            each(code_and_leave, c + AHEAD)

        each(decode, c - LAG)

        @pl.when(c == CHUNKS // 2)
        def _():
            serve_rows()

        return 0

    lax.fori_loop(LAG, CHUNKS, step, 0)
    for c in range(CHUNKS - LAG, CHUNKS - 1):
        each(decode, c)
    columns = pl.ds(0, 48)
    wait(router.at[columns], row_recv_sem)
    wait(router.at[columns], row_send_sem)
    wait(squares.at[1, rest], mate_send_sem)
    wait(parts.at[0, 0, three], parts_send_sem.at[0])
    wait(parts.at[0, three], parts_send_sem.at[1])
    wait(parts.at[0], parts_send_sem.at[2])
    wait(sums_send.at[three], sums_send_sem)
    wait(sums_recv.at[pl.ds(0, 7)], sums_pass_sem)
    every = pl.ds(0, PAIRS)
    wait(send.at[every, three], send_sem)
    for p in range(PAIRS - 2, PAIRS):
        wait(recv.at[p, pl.ds(0, 7)], recv_sem.at[p])
    wait(recv.at[every, pl.ds(0, 7)], pass_sem)


def hand_out(
    out, begun, router, recv, table,
    gate, up, down, sg, su, sd, served,
    last, totals, scale, wide_rows, sem,
):
    few = 4
    copies = []

    def copy(src, dst):
        copies.append(pltpu.make_async_copy(src, dst, sem.at[len(copies)]))
        copies[-1].start()

    for a, big in enumerate((gate, up, down)):
        count = 16 - few * (a == 2)
        copy(out.at[pl.ds(16 * a, count)], big.at[pl.ds(0, count)])
    copy(router, served)
    totals[...] = begun[...]

    def go(i, _):
        decode_pair(recv, table, last, totals, wide_rows, PAIRS - 2 + i, i)
        return 0

    lax.fori_loop(0, 2, go, 0)
    copy(last, down.at[pl.ds(16 - few, few)])
    across = jnp.concatenate([totals[...], jnp.zeros((96, 128), jnp.float32)], axis=0).T
    scale[...] = jnp.sqrt(across[0:48, 0:32])
    for a, small in enumerate((sg, su, sd)):
        copy(scale.at[pl.ds(16 * a, 16)], small)
    for c in copies:
        c.wait()


def body(gate, up, down, weight, gain):
    vmem = pl.BlockSpec(memory_space=pltpu.VMEM)
    hbm = pl.BlockSpec(memory_space=pltpu.HBM)
    f32, bf16 = jnp.float32, jnp.bfloat16
    dma = pltpu.SemaphoreType.DMA
    results = pl.pallas_call(
        exchange,
        name="exchange",
        out_shape=(
            pltpu.VMEM((48, 32, 2048), bf16),
            pltpu.VMEM((32, 128), f32),
            pltpu.VMEM((64, 2048), bf16),
            pltpu.VMEM((PAIRS, 8, 4, 32, 128), bf16),
            pltpu.VMEM((48, 32, 128), f32),
        ),
        in_specs=[hbm, hbm, hbm, vmem, vmem],
        out_specs=(vmem,) * 5,
        scratch_shapes=[
            pltpu.VMEM((48, 64, 1024), f32),
            pltpu.VMEM((PAIRS, 4, 8, 32, 128), bf16),
            pltpu.VMEM((PAIRS, 4, 8, 32, 128), bf16),
            pltpu.VMEM((2, 48, 1, 1024), f32),
            pltpu.VMEM((48, 1, 1024), f32),
            pltpu.VMEM((4, 8, 8, 128), bf16),
            pltpu.VMEM((4, 8, 8, 128), bf16),
            pltpu.VMEM((8, 4, 8, 128), bf16),
            pltpu.VMEM((2, 4, 4, 8, 128), bf16),
            pltpu.VMEM((2, 32, 2048), f32),
            dma((5,)),
            dma,
            dma((PAIRS,)),
            dma,
            dma((PAIRS,)),
            dma,
            dma,
            dma,
            dma,
            dma((3,)),
            dma((3,)),
            dma,
            dma,
            dma,
            dma,
        ],
        compiler_params=pltpu.CompilerParams(
            collective_id=0, has_side_effects=True, vmem_limit_bytes=49 * 2**20
        ),
    )(gate, up, jnp.swapaxes(down, 1, 2), weight.T, gain.reshape(1, 64))
    half = jax.ShapeDtypeStruct((16, 32, 2048), bf16)
    few = jax.ShapeDtypeStruct((16, 32), f32)
    gate, up, down, sg, su, sd, served = pl.pallas_call(
        hand_out,
        name="hand_out",
        out_shape=(half, half, half, few, few, few, jax.ShapeDtypeStruct((64, 2048), bf16)),
        in_specs=[vmem] * 5,
        out_specs=(hbm,) * 7,
        scratch_shapes=[
            pltpu.VMEM((4, 32, 2048), bf16),
            pltpu.VMEM((32, 128), f32),
            pltpu.VMEM((48, 32), f32),
            pltpu.VMEM((2, 32, 2048), f32),
            dma((8,)),
        ],
        compiler_params=pltpu.CompilerParams(vmem_limit_bytes=16 * 2**20),
    )(*(pltpu.with_memory_space_constraint(a, pltpu.VMEM) for a in results))
    return (
        jnp.swapaxes(gate, 1, 2),
        jnp.swapaxes(up, 1, 2),
        down,
        sg,
        su,
        sd,
        served.T,
    )


def solution(mesh):
    return jax.shard_map(
        body,
        mesh=mesh,
        in_specs=(
            P("bank", "zero", None),
            P("bank", "zero", None),
            P("bank", None, "zero"),
            P("zero", "bank"),
            P("zero"),
        ),
        out_specs=(
            P("bank", None, "zero"),
            P("bank", None, "zero"),
            P("bank", "zero", None),
            P("bank", "zero"),
            P("bank", "zero"),
            P("bank", "zero"),
            P(),
        ),
        check_vma=False,
    )
```

```python
import jax
import jax.numpy as jnp
from jax import lax
from jax.experimental import pallas as pl
from jax.experimental.pallas import tpu as pltpu
from jax.sharding import PartitionSpec as P

MESH = pl.DeviceIdType.MESH
CHUNKS = 12
OWN, SHARED = 16, 16
LAG = 4
AHEAD = 6
PAIRS = 24
POWER = 20
UP = 2.0**6.25


def turned(h, a, b):
    return a + h * (b - a), b + h * (a - b)


def left_half():
    return lax.broadcasted_iota(jnp.int32, (32, 128), 1) < 64


def decode_pair(recv, table, out, totals, wide, p, place):
    half = left_half()
    h = lax.rem(p, 2)
    f0 = table[2 * p]
    f1 = table[2 * p + 1]
    squares = [jnp.zeros((32, 128), jnp.float32)] * 2
    for t in range(16):
        z, x = t // 4, t % 4
        one, two = turned(h, z, x)
        left, right = 8 * z + x, 8 * z + 4 + x
        columns = slice(128 * t, 128 * t + 128)
        a = recv[p, 2 * one, two].astype(jnp.float32)
        b = recv[p, 2 * one + 1, two].astype(jnp.float32)
        for e, f, u in (
            (0, f0, jnp.where(half, a, pltpu.roll(b, 64, 1))),
            (1, f1, jnp.where(half, pltpu.roll(a, 64, 1), b)),
        ):
            g = jnp.where(
                half,
                jnp.broadcast_to(f[:, left : left + 1], (32, 128)),
                jnp.broadcast_to(f[:, right : right + 1], (32, 128)),
            )
            m = jnp.exp(jnp.log(jnp.abs(u)) * (1.0 / POWER))
            v = jnp.where(u < 0.0, -m, m) * g
            wide[e, :, columns] = v
            squares[e] = squares[e] + v * v
    lane = lax.broadcasted_iota(jnp.int32, (32, 128), 1)
    for e in range(2):
        total = jnp.sum(squares[e], axis=1, keepdims=True)
        totals[...] = jnp.where(lane == 2 * p + e, total, totals[...])
        r = lax.rsqrt(total)
        for t in range(16):
            columns = slice(128 * t, 128 * t + 128)
            out[2 * place + e, :, columns] = (wide[e, :, columns] * r).astype(jnp.bfloat16)


def exchange(
    gate, up, down, weight, gain,
    out, totals, router, recv, table,
    xin, send, relay, squares, sums, sums_send, sums_relay, sums_recv, parts, wide_rows,
    in_sem, send_sem, relay_sem, pass_sem, recv_sem,
    sums_send_sem, sums_relay_sem, sums_pass_sem, sums_recv_sem,
    parts_send_sem, parts_recv_sem, row_send_sem, row_recv_sem,
    mate_send_sem, mate_recv_sem,
):
    me = lax.axis_index("zero")
    bank = lax.axis_index("bank")
    mz, mx, mc = lax.div(me, 8), lax.rem(lax.div(me, 2), 4), lax.rem(me, 2)
    mate = 1 - mc

    def turn(place, i):
        return lax.rem(place + i, 4)

    def device(z, x, c):
        return z * 8 + x * 2 + c

    def put(src, dst, sent, arrived, z, x, c):
        pltpu.make_async_remote_copy(
            src_ref=src,
            dst_ref=dst,
            send_sem=sent,
            recv_sem=arrived,
            device_id={"zero": device(z, x, c)},
            device_id_type=MESH,
        ).start()

    def wait(ref, sem):
        pltpu.make_async_copy(ref, ref, sem).wait()

    barrier = pltpu.get_barrier_semaphore()

    def greet(**where):
        pl.semaphore_signal(
            barrier, inc=1, device_id=where, device_id_type=MESH
        )

    for i in (2, 1, 3):
        for c in range(2):
            greet(zero=device(turn(mz, i), mx, c))
            greet(zero=device(mz, turn(mx, i), c))
        greet(bank=turn(bank, i))
    greet(zero=device(mz, mx, mate))

    loads = [
        pltpu.make_async_copy(
            ref.at[pl.ds(k, count)], xin.at[pl.ds(16 * a + k, count)], in_sem.at[i]
        )
        for i, (a, ref, k, count) in enumerate(((0, gate, 0, 4), (0, gate, 4, 4), (0, gate, 8, 8), (1, up, 0, 16), (2, down, 0, 16)))
    ]
    for copy in loads[:2]:
        copy.start()

    part = (weight[...] * gain[...]).astype(jnp.bfloat16)
    parts[mc, mz, mx] = jnp.concatenate([part[0:8], part[8:16]], axis=1)

    def add_up(e, _):
        x = xin[e]
        squares[0, e] = jnp.sum(x * x, axis=0, keepdims=True)
        return 0

    def own_norm(e, _):
        x = xin[e]
        norm = jnp.sqrt(jnp.sum(x * x, axis=0, keepdims=True))
        sums[e] = norm.astype(jnp.bfloat16).astype(jnp.float32)
        return 0

    def chip_norm(e, _):
        norm = jnp.sqrt(squares[0, e] + squares[1, e])
        sums[e] = norm.astype(jnp.bfloat16).astype(jnp.float32)
        return 0

    def code(p):
        h = lax.rem(p, 2)
        for b in range(8):
            columns = slice(128 * b, 128 * b + 128)
            halves = []
            for e in range(2):
                s = sums[2 * p + e, :, columns]
                r = jnp.where(s > 0.0, UP / s, 0.0)
                halves.append(xin[2 * p + e, :, columns] * r)
            y = jnp.concatenate(halves, axis=0).T
            y2 = y * y
            y4 = y2 * y2
            y8 = y4 * y4
            y20 = y8 * y8 * y4
            u = jnp.where(y < 0.0, -y20, y20).astype(jnp.bfloat16)
            for q in range(4):
                z, x, d = b // 2, b % 2 * 2 + q // 2, q % 2
                first, second = turned(h, x, z)
                send[p, first, 2 * second + d] = u[32 * q : 32 * q + 32]

    def leave(p):
        h = lax.rem(p, 2)
        mine, other = turned(h, mx, mz)
        for i in (2, 1, 3):
            to = turn(mine, i)
            x, z = turned(h, to, other)
            put(send.at[p, to], relay.at[p, mine], send_sem, relay_sem.at[p], z, x, mc)
        relay[p, mine] = send[p, mine]

    four = pl.ds(0, 4)
    three = pl.ds(0, 3)

    def go_on(p):
        h = lax.rem(p, 2)
        wait(relay.at[p, three], relay_sem.at[p])
        mine, other = turned(h, mz, mx)
        slot = 2 * mine + mc
        put(relay.at[p, four, 2 * mine + mate], recv.at[p, slot], pass_sem, recv_sem.at[p], mz, mx, mate)
        for i in (2, 1, 3):
            to = turn(mine, i)
            z, x = turned(h, to, other)
            for d in range(2):
                put(relay.at[p, four, 2 * to + d], recv.at[p, slot], pass_sem, recv_sem.at[p], z, x, d)
        recv[p, slot] = relay[p, :, slot]

    def each(act, c):
        def go(p, _):
            act(p)
            return 0

        lax.fori_loop(2 * c, 2 * c + 2, go, 0)

    def code_and_leave(p):
        code(p)
        leave(p)

    loads[0].wait()
    lax.fori_loop(0, 4, own_norm, 0)
    each(code, 0)
    pl.semaphore_wait(barrier, 16)
    each(leave, 0)
    for copy in loads[2:]:
        copy.start()
    loads[1].wait()
    lax.fori_loop(4, 8, own_norm, 0)
    each(code_and_leave, 1)
    loads[2].wait()
    lax.fori_loop(8, OWN, own_norm, 0)
    each(code_and_leave, 2)
    each(code_and_leave, 3)

    for copy, low, high in zip(loads[3:], (16, 32), (32, 48)):
        copy.wait()
        lax.fori_loop(low, high, add_up, 0)
    rest = pl.ds(OWN, 48 - OWN)
    put(squares.at[0, rest], squares.at[1, rest], mate_send_sem, mate_recv_sem, mz, mx, mate)
    each(go_on, 0)
    wait(squares.at[1, rest], mate_recv_sem)
    lax.fori_loop(OWN, 48, chip_norm, 0)

    for b in range(8):
        columns = slice(128 * b, 128 * b + 128)
        s = jnp.concatenate(
            [
                sums[0:OWN, 0, columns],
                sums[pl.ds(OWN + SHARED * mc, SHARED), 0, columns],
            ],
            axis=0,
        )
        t = jnp.concatenate(
            [s] + [pltpu.roll(s, 128 - 8 * g, 1) for g in range(1, 4)], axis=0
        ).T
        for q in range(4):
            z, x, d = b // 2, b % 2 * 2 + q // 2, q % 2
            sums_send[x, 2 * z + d] = t[32 * q : 32 * q + 8].astype(jnp.bfloat16)
    for i in (1, 3, 2):
        x = turn(mx, i)
        put(sums_send.at[x], sums_relay.at[mx], sums_send_sem, sums_relay_sem, mz, x, mc)
        put(parts.at[mc, mz, mx], parts.at[mc, mz, mx], parts_send_sem.at[0], parts_recv_sem.at[0], mz, x, mc)
    sums_relay[mx] = sums_send[mx]

    for c in range(4, AHEAD + 1):
        each(code_and_leave, c)
    each(go_on, 1)
    each(code_and_leave, AHEAD + 1)

    wait(sums_relay.at[three], sums_relay_sem)
    wait(parts.at[0, 0, three], parts_recv_sem.at[0])
    at_z = 2 * mz + mc
    for i in (1, 3, 2):
        z = turn(mz, i)
        for d in range(2):
            put(sums_relay.at[four, 2 * z + d], sums_recv.at[at_z], sums_pass_sem, sums_recv_sem, z, mx, d)
        put(parts.at[mc, mz], parts.at[mc, mz], parts_send_sem.at[1], parts_recv_sem.at[1], z, mx, mc)
    put(sums_relay.at[four, 2 * mz + mate], sums_recv.at[at_z], sums_pass_sem, sums_recv_sem, mz, mx, mate)
    sums_recv[at_z] = sums_relay[:, at_z]

    for c in range(2, LAG):
        each(go_on, c)
        each(code_and_leave, AHEAD + c)

    wait(sums_recv.at[pl.ds(0, 7)], sums_recv_sem)
    wide = sums_recv[...].astype(jnp.float32).reshape(32, 8, 128)
    core = lax.rem(lax.div(lax.broadcasted_iota(jnp.int32, (128, 128), 1), 4), 2)
    for n in range(8):
        rows = jnp.concatenate([wide[:, n, :], jnp.zeros((96, 128), jnp.float32)], axis=0).T
        rows = rows * (1.0 / UP)
        low = jnp.where(core == 0, rows, pltpu.roll(rows, 4, 1))
        high = jnp.where(core == 1, rows, pltpu.roll(rows, 124, 1))
        for g in range(4):
            place = n + 8 * g
            own, chip = 32 * g, 32 * g + OWN
            table[0:OWN, place, :] = rows[own:chip]
            table[OWN : OWN + SHARED, place, :] = low[chip : chip + SHARED]
            table[OWN + SHARED : 48, place, :] = high[chip : chip + SHARED]
    totals[...] = jnp.zeros_like(totals)

    half = left_half()

    def decode(p):
        wait(recv.at[p, pl.ds(0, 7)], recv_sem.at[p])
        decode_pair(recv, table, out, totals, wide_rows, p, p)

    wait(parts.at[0, three], parts_recv_sem.at[1])
    put(parts.at[mc], parts.at[mc], parts_send_sem.at[2], parts_recv_sem.at[2], mz, mx, mate)

    mine = pl.ds(pl.multiple_of(16 * bank, 16), 16)

    def serve_rows():
        wait(parts.at[0], parts_recv_sem.at[2])
        low = half[0:8]
        for t in range(16):
            z, x = t // 4, t % 4
            a = parts[0, z, x].astype(jnp.float32)
            b = parts[1, z, x].astype(jnp.float32)
            block = jnp.concatenate(
                [
                    jnp.where(low, a, pltpu.roll(b, 64, 1)),
                    jnp.where(low, pltpu.roll(a, 64, 1), b),
                ],
                axis=0,
            )
            router[mine, 128 * t : 128 * t + 128] = block.astype(jnp.bfloat16)
        for i in range(1, 4):
            pltpu.make_async_remote_copy(
                src_ref=router.at[mine],
                dst_ref=router.at[mine],
                send_sem=row_send_sem,
                recv_sem=row_recv_sem,
                device_id={"bank": turn(bank, i)},
                device_id_type=MESH,
            ).start()

    def step(c, _):
        each(go_on, c)

        @pl.when(c < CHUNKS - AHEAD)
        def _():
            each(code_and_leave, c + AHEAD)

        each(decode, c - LAG)

        @pl.when(c == CHUNKS // 2)
        def _():
            serve_rows()

        return 0

    lax.fori_loop(LAG, CHUNKS, step, 0)
    for c in range(CHUNKS - LAG, CHUNKS - 1):
        each(decode, c)
    columns = pl.ds(0, 48)
    wait(router.at[columns], row_recv_sem)
    wait(router.at[columns], row_send_sem)
    wait(squares.at[1, rest], mate_send_sem)
    wait(parts.at[0, 0, three], parts_send_sem.at[0])
    wait(parts.at[0, three], parts_send_sem.at[1])
    wait(parts.at[0], parts_send_sem.at[2])
    wait(sums_send.at[three], sums_send_sem)
    wait(sums_recv.at[pl.ds(0, 7)], sums_pass_sem)
    every = pl.ds(0, PAIRS)
    wait(send.at[every, three], send_sem)
    for p in range(PAIRS - 2, PAIRS):
        wait(recv.at[p, pl.ds(0, 7)], recv_sem.at[p])
    wait(recv.at[every, pl.ds(0, 7)], pass_sem)


def hand_out(
    out, begun, router, recv, table,
    gate, up, down, sg, su, sd, served,
    last, totals, scale, wide_rows, sem,
):
    few = 4
    copies = []

    def copy(src, dst):
        copies.append(pltpu.make_async_copy(src, dst, sem.at[len(copies)]))
        copies[-1].start()

    for a, big in enumerate((gate, up, down)):
        count = 16 - few * (a == 2)
        copy(out.at[pl.ds(16 * a, count)], big.at[pl.ds(0, count)])
    copy(router, served)
    totals[...] = begun[...]

    def go(i, _):
        decode_pair(recv, table, last, totals, wide_rows, PAIRS - 2 + i, i)
        return 0

    lax.fori_loop(0, 2, go, 0)
    copy(last, down.at[pl.ds(16 - few, few)])
    across = jnp.concatenate([totals[...], jnp.zeros((96, 128), jnp.float32)], axis=0).T
    scale[...] = jnp.sqrt(across[0:48, 0:32])
    for a, small in enumerate((sg, su, sd)):
        copy(scale.at[pl.ds(16 * a, 16)], small)
    for c in copies:
        c.wait()


def body(gate, up, down, weight, gain):
    vmem = pl.BlockSpec(memory_space=pltpu.VMEM)
    hbm = pl.BlockSpec(memory_space=pltpu.HBM)
    f32, bf16 = jnp.float32, jnp.bfloat16
    dma = pltpu.SemaphoreType.DMA
    results = pl.pallas_call(
        exchange,
        name="exchange",
        out_shape=(
            pltpu.VMEM((48, 32, 2048), bf16),
            pltpu.VMEM((32, 128), f32),
            pltpu.VMEM((64, 2048), bf16),
            pltpu.VMEM((PAIRS, 8, 4, 32, 128), bf16),
            pltpu.VMEM((48, 32, 128), f32),
        ),
        in_specs=[hbm, hbm, hbm, vmem, vmem],
        out_specs=(vmem,) * 5,
        scratch_shapes=[
            pltpu.VMEM((48, 64, 1024), f32),
            pltpu.VMEM((PAIRS, 4, 8, 32, 128), bf16),
            pltpu.VMEM((PAIRS, 4, 8, 32, 128), bf16),
            pltpu.VMEM((2, 48, 1, 1024), f32),
            pltpu.VMEM((48, 1, 1024), f32),
            pltpu.VMEM((4, 8, 8, 128), bf16),
            pltpu.VMEM((4, 8, 8, 128), bf16),
            pltpu.VMEM((8, 4, 8, 128), bf16),
            pltpu.VMEM((2, 4, 4, 8, 128), bf16),
            pltpu.VMEM((2, 32, 2048), f32),
            dma((5,)),
            dma,
            dma((PAIRS,)),
            dma,
            dma((PAIRS,)),
            dma,
            dma,
            dma,
            dma,
            dma((3,)),
            dma((3,)),
            dma,
            dma,
            dma,
            dma,
        ],
        compiler_params=pltpu.CompilerParams(
            collective_id=0, has_side_effects=True, vmem_limit_bytes=49 * 2**20
        ),
    )(gate, up, jnp.swapaxes(down, 1, 2), weight.T, gain.reshape(1, 64))
    half = jax.ShapeDtypeStruct((16, 32, 2048), bf16)
    few = jax.ShapeDtypeStruct((16, 32), f32)
    gate, up, down, sg, su, sd, served = pl.pallas_call(
        hand_out,
        name="hand_out",
        out_shape=(half, half, half, few, few, few, jax.ShapeDtypeStruct((64, 2048), bf16)),
        in_specs=[vmem] * 5,
        out_specs=(hbm,) * 7,
        scratch_shapes=[
            pltpu.VMEM((4, 32, 2048), bf16),
            pltpu.VMEM((32, 128), f32),
            pltpu.VMEM((48, 32), f32),
            pltpu.VMEM((2, 32, 2048), f32),
            dma((8,)),
        ],
        compiler_params=pltpu.CompilerParams(vmem_limit_bytes=16 * 2**20),
    )(*(pltpu.with_memory_space_constraint(a, pltpu.VMEM) for a in results))
    return (
        jnp.swapaxes(gate, 1, 2),
        jnp.swapaxes(up, 1, 2),
        down,
        sg,
        su,
        sd,
        served.T,
    )


def solution(mesh):
    return jax.shard_map(
        body,
        mesh=mesh,
        in_specs=(
            P("bank", "zero", None),
            P("bank", "zero", None),
            P("bank", None, "zero"),
            P("zero", "bank"),
            P("zero"),
        ),
        out_specs=(
            P("bank", None, "zero"),
            P("bank", None, "zero"),
            P("bank", "zero", None),
            P("bank", "zero"),
            P("bank", "zero"),
            P("bank", "zero"),
            P(),
        ),
        check_vma=False,
    )
```

```python
import jax
import jax.numpy as jnp
from jax import lax
from jax.experimental import pallas as pl
from jax.experimental.pallas import tpu as pltpu
from jax.sharding import PartitionSpec as P

MESH = pl.DeviceIdType.MESH
CHUNKS = 12
OWN, SHARED = 16, 16
LAG = 4
AHEAD = 4
PAIRS = 24
POWER = 20
UP = 2.0**6.25


def turned(h, a, b):
    return a + h * (b - a), b + h * (a - b)


def left_half():
    return lax.broadcasted_iota(jnp.int32, (32, 128), 1) < 64


def decode_pair(recv, table, out, totals, wide, p, place):
    half = left_half()
    h = lax.rem(p, 2)
    f0 = table[2 * p]
    f1 = table[2 * p + 1]
    squares = [jnp.zeros((32, 128), jnp.float32)] * 2
    for t in range(16):
        z, x = t // 4, t % 4
        one, two = turned(h, z, x)
        left, right = 8 * z + x, 8 * z + 4 + x
        columns = slice(128 * t, 128 * t + 128)
        a = recv[p, 2 * one, two].astype(jnp.float32)
        b = recv[p, 2 * one + 1, two].astype(jnp.float32)
        for e, f, u in (
            (0, f0, jnp.where(half, a, pltpu.roll(b, 64, 1))),
            (1, f1, jnp.where(half, pltpu.roll(a, 64, 1), b)),
        ):
            g = jnp.where(
                half,
                jnp.broadcast_to(f[:, left : left + 1], (32, 128)),
                jnp.broadcast_to(f[:, right : right + 1], (32, 128)),
            )
            m = jnp.exp(jnp.log(jnp.abs(u)) * (1.0 / POWER))
            v = jnp.where(u < 0.0, -m, m) * g
            wide[e, :, columns] = v
            squares[e] = squares[e] + v * v
    lane = lax.broadcasted_iota(jnp.int32, (32, 128), 1)
    for e in range(2):
        total = jnp.sum(squares[e], axis=1, keepdims=True)
        totals[...] = jnp.where(lane == 2 * p + e, total, totals[...])
        r = lax.rsqrt(total)
        for t in range(16):
            columns = slice(128 * t, 128 * t + 128)
            out[2 * place + e, :, columns] = (wide[e, :, columns] * r).astype(jnp.bfloat16)


def exchange(
    gate, up, down, weight, gain,
    out, totals, router, recv, table,
    xin, send, relay, squares, sums, sums_send, sums_relay, sums_recv, parts, wide_rows,
    in_sem, send_sem, relay_sem, pass_sem, recv_sem,
    sums_send_sem, sums_relay_sem, sums_pass_sem, sums_recv_sem,
    parts_send_sem, parts_recv_sem, row_send_sem, row_recv_sem,
    mate_send_sem, mate_recv_sem,
):
    me = lax.axis_index("zero")
    bank = lax.axis_index("bank")
    mz, mx, mc = lax.div(me, 8), lax.rem(lax.div(me, 2), 4), lax.rem(me, 2)
    mate = 1 - mc

    def turn(place, i):
        return lax.rem(place + i, 4)

    def device(z, x, c):
        return z * 8 + x * 2 + c

    def put(src, dst, sent, arrived, z, x, c):
        pltpu.make_async_remote_copy(
            src_ref=src,
            dst_ref=dst,
            send_sem=sent,
            recv_sem=arrived,
            device_id={"zero": device(z, x, c)},
            device_id_type=MESH,
        ).start()

    def wait(ref, sem):
        pltpu.make_async_copy(ref, ref, sem).wait()

    loads = [
        pltpu.make_async_copy(
            ref.at[pl.ds(k, count)], xin.at[pl.ds(16 * a + k, count)], in_sem.at[i]
        )
        for i, (a, ref, k, count) in enumerate(((0, gate, 0, 4), (0, gate, 4, 4), (0, gate, 8, 8), (1, up, 0, 16), (2, down, 0, 16)))
    ]
    for copy in loads[:2]:
        copy.start()

    barrier = pltpu.get_barrier_semaphore()

    def greet(**where):
        pl.semaphore_signal(
            barrier, inc=1, device_id=where, device_id_type=MESH
        )

    greet(zero=device(mz, mx, mate))
    for i in (1, 3, 2):
        for c in range(2):
            greet(zero=device(turn(mz, i), mx, c))
            greet(zero=device(mz, turn(mx, i), c))
        greet(bank=turn(bank, i))

    part = (weight[...] * gain[...]).astype(jnp.bfloat16)
    row, spot = turned(mc, mz, mx)
    parts[mc, row, spot] = jnp.concatenate([part[0:8], part[8:16]], axis=1)

    def add_up(e, _):
        x = xin[e]
        squares[0, e] = jnp.sum(x * x, axis=0, keepdims=True)
        return 0

    def own_norm(e, _):
        sums[e] = jnp.sqrt(squares[0, e]).astype(jnp.bfloat16).astype(jnp.float32)
        return 0

    def chip_norm(e, _):
        norm = jnp.sqrt(squares[0, e] + squares[1, e])
        sums[e] = norm.astype(jnp.bfloat16).astype(jnp.float32)
        return 0

    def code(p):
        h = lax.rem(p, 2)
        for b in range(8):
            columns = slice(128 * b, 128 * b + 128)
            halves = []
            for e in range(2):
                s = sums[2 * p + e, :, columns]
                r = jnp.where(s > 0.0, UP / s, 0.0)
                halves.append(xin[2 * p + e, :, columns] * r)
            y = jnp.concatenate(halves, axis=0).T
            y2 = y * y
            y4 = y2 * y2
            y8 = y4 * y4
            y20 = y8 * y8 * y4
            u = jnp.where(y < 0.0, -y20, y20).astype(jnp.bfloat16)
            for q in range(4):
                z, x, d = b // 2, b % 2 * 2 + q // 2, q % 2
                first, second = turned(h, x, z)
                send[p, first, 2 * second + d] = u[32 * q : 32 * q + 32]

    def leave(p):
        h = lax.rem(p, 2)
        mine, other = turned(h, mx, mz)
        for i in (2, 1, 3):
            to = turn(mine, i)
            x, z = turned(h, to, other)
            put(send.at[p, to], relay.at[p, mine], send_sem, relay_sem.at[p], z, x, mc)
        relay[p, mine] = send[p, mine]

    four = pl.ds(0, 4)
    three = pl.ds(0, 3)

    def go_on(p):
        h = lax.rem(p, 2)
        wait(relay.at[p, three], relay_sem.at[p])
        mine, other = turned(h, mz, mx)
        slot = 2 * mine + mc
        put(relay.at[p, four, 2 * mine + mate], recv.at[p, slot], pass_sem, recv_sem.at[p], mz, mx, mate)
        for i in (2, 1, 3):
            to = turn(mine, i)
            z, x = turned(h, to, other)
            for d in range(2):
                put(relay.at[p, four, 2 * to + d], recv.at[p, slot], pass_sem, recv_sem.at[p], z, x, d)
        recv[p, slot] = relay[p, :, slot]

    def each(act, c):
        def go(p, _):
            act(p)
            return 0

        lax.fori_loop(2 * c, 2 * c + 2, go, 0)

    def code_and_leave(p):
        code(p)
        leave(p)

    loads[0].wait()
    lax.fori_loop(0, 4, add_up, 0)
    lax.fori_loop(0, 4, own_norm, 0)
    each(code, 0)
    pl.semaphore_wait(barrier, 16)
    each(leave, 0)
    for copy in loads[2:]:
        copy.start()
    loads[1].wait()
    lax.fori_loop(4, 8, add_up, 0)
    lax.fori_loop(4, 8, own_norm, 0)
    each(code_and_leave, 1)
    loads[2].wait()
    lax.fori_loop(8, OWN, add_up, 0)
    lax.fori_loop(8, OWN, own_norm, 0)
    each(code_and_leave, 2)
    each(code_and_leave, 3)

    for copy, low, high in zip(loads[3:], (16, 32), (32, 48)):
        copy.wait()
        lax.fori_loop(low, high, add_up, 0)
    rest = pl.ds(OWN, 48 - OWN)
    put(squares.at[0, rest], squares.at[1, rest], mate_send_sem, mate_recv_sem, mz, mx, mate)
    each(go_on, 0)
    wait(squares.at[1, rest], mate_recv_sem)
    lax.fori_loop(OWN, 48, chip_norm, 0)

    for b in range(8):
        columns = slice(128 * b, 128 * b + 128)
        s = jnp.concatenate(
            [
                sums[0:OWN, 0, columns],
                sums[pl.ds(OWN + SHARED * mc, SHARED), 0, columns],
            ],
            axis=0,
        )
        t = jnp.concatenate(
            [s] + [pltpu.roll(s, 128 - 8 * g, 1) for g in range(1, 4)], axis=0
        ).T
        for q in range(4):
            z, x, d = b // 2, b % 2 * 2 + q // 2, q % 2
            sums_send[x, 2 * z + d] = t[32 * q : 32 * q + 8].astype(jnp.bfloat16)
    for i in (1, 3, 2):
        x = turn(mx, i)
        put(sums_send.at[x], sums_relay.at[mx], sums_send_sem, sums_relay_sem, mz, x, mc)
        z_to, x_to = turned(mc, row, turn(spot, i))
        put(parts.at[mc, row, spot], parts.at[mc, row, spot], parts_send_sem.at[0], parts_recv_sem.at[0], z_to, x_to, mc)
    sums_relay[mx] = sums_send[mx]

    each(code_and_leave, AHEAD)
    each(go_on, 1)
    each(code_and_leave, AHEAD + 1)

    wait(sums_relay.at[three], sums_relay_sem)
    wait(parts.at[0, 0, three], parts_recv_sem.at[0])
    at_z = 2 * mz + mc
    for i in (1, 3, 2):
        z = turn(mz, i)
        for d in range(2):
            put(sums_relay.at[four, 2 * z + d], sums_recv.at[at_z], sums_pass_sem, sums_recv_sem, z, mx, d)
        z_to, x_to = turned(mc, turn(row, i), spot)
        put(parts.at[mc, row], parts.at[mc, row], parts_send_sem.at[1], parts_recv_sem.at[1], z_to, x_to, mc)
    put(sums_relay.at[four, 2 * mz + mate], sums_recv.at[at_z], sums_pass_sem, sums_recv_sem, mz, mx, mate)
    sums_recv[at_z] = sums_relay[:, at_z]

    for c in range(2, LAG):
        each(go_on, c)
        each(code_and_leave, AHEAD + c)

    wait(sums_recv.at[pl.ds(0, 7)], sums_recv_sem)
    wide = sums_recv[...].astype(jnp.float32).reshape(32, 8, 128)
    core = lax.rem(lax.div(lax.broadcasted_iota(jnp.int32, (128, 128), 1), 4), 2)
    for n in range(8):
        rows = jnp.concatenate([wide[:, n, :], jnp.zeros((96, 128), jnp.float32)], axis=0).T
        rows = rows * (1.0 / UP)
        low = jnp.where(core == 0, rows, pltpu.roll(rows, 4, 1))
        high = jnp.where(core == 1, rows, pltpu.roll(rows, 124, 1))
        for g in range(4):
            place = n + 8 * g
            own, chip = 32 * g, 32 * g + OWN
            table[0:OWN, place, :] = rows[own:chip]
            table[OWN : OWN + SHARED, place, :] = low[chip : chip + SHARED]
            table[OWN + SHARED : 48, place, :] = high[chip : chip + SHARED]
    totals[...] = jnp.zeros_like(totals)

    half = left_half()

    def decode(p):
        wait(recv.at[p, pl.ds(0, 7)], recv_sem.at[p])
        decode_pair(recv, table, out, totals, wide_rows, p, p)

    wait(parts.at[0, three], parts_recv_sem.at[1])
    put(parts.at[mc], parts.at[mc], parts_send_sem.at[2], parts_recv_sem.at[2], mz, mx, mate)

    mine = pl.ds(pl.multiple_of(16 * bank, 16), 16)

    def serve_rows():
        wait(parts.at[0], parts_recv_sem.at[2])
        low = half[0:8]
        for t in range(16):
            z, x = t // 4, t % 4
            a = parts[0, z, x].astype(jnp.float32)
            b = parts[1, x, z].astype(jnp.float32)
            block = jnp.concatenate(
                [
                    jnp.where(low, a, pltpu.roll(b, 64, 1)),
                    jnp.where(low, pltpu.roll(a, 64, 1), b),
                ],
                axis=0,
            )
            router[mine, 128 * t : 128 * t + 128] = block.astype(jnp.bfloat16)
        for i in range(1, 4):
            pltpu.make_async_remote_copy(
                src_ref=router.at[mine],
                dst_ref=router.at[mine],
                send_sem=row_send_sem,
                recv_sem=row_recv_sem,
                device_id={"bank": turn(bank, i)},
                device_id_type=MESH,
            ).start()

    def step(c, _):
        each(go_on, c)

        @pl.when(c < CHUNKS - AHEAD)
        def _():
            each(code_and_leave, c + AHEAD)

        each(decode, c - LAG)

        @pl.when(c == CHUNKS // 2)
        def _():
            serve_rows()

        return 0

    lax.fori_loop(LAG, CHUNKS, step, 0)
    for c in range(CHUNKS - LAG, CHUNKS - 1):
        each(decode, c)
    columns = pl.ds(0, 48)
    wait(router.at[columns], row_recv_sem)
    wait(router.at[columns], row_send_sem)
    wait(squares.at[1, rest], mate_send_sem)
    wait(parts.at[0, 0, three], parts_send_sem.at[0])
    wait(parts.at[0, three], parts_send_sem.at[1])
    wait(parts.at[0], parts_send_sem.at[2])
    wait(sums_send.at[three], sums_send_sem)
    wait(sums_recv.at[pl.ds(0, 7)], sums_pass_sem)
    every = pl.ds(0, PAIRS)
    wait(send.at[every, three], send_sem)
    for p in range(PAIRS - 2, PAIRS):
        wait(recv.at[p, pl.ds(0, 7)], recv_sem.at[p])
    wait(recv.at[every, pl.ds(0, 7)], pass_sem)


def hand_out(
    out, begun, router, recv, table,
    gate, up, down, sg, su, sd, served,
    last, totals, scale, wide_rows, sem,
):
    few = 4
    copies = []

    def copy(src, dst):
        copies.append(pltpu.make_async_copy(src, dst, sem.at[len(copies)]))
        copies[-1].start()

    for a, big in enumerate((gate, up, down)):
        count = 16 - few * (a == 2)
        copy(out.at[pl.ds(16 * a, count)], big.at[pl.ds(0, count)])
    copy(router, served)
    totals[...] = begun[...]

    def go(i, _):
        decode_pair(recv, table, last, totals, wide_rows, PAIRS - 2 + i, i)
        return 0

    lax.fori_loop(0, 2, go, 0)
    copy(last, down.at[pl.ds(16 - few, few)])
    across = jnp.concatenate([totals[...], jnp.zeros((96, 128), jnp.float32)], axis=0).T
    scale[...] = jnp.sqrt(across[0:48, 0:32])
    for a, small in enumerate((sg, su, sd)):
        copy(scale.at[pl.ds(16 * a, 16)], small)
    for c in copies:
        c.wait()


def body(gate, up, down, weight, gain):
    vmem = pl.BlockSpec(memory_space=pltpu.VMEM)
    hbm = pl.BlockSpec(memory_space=pltpu.HBM)
    f32, bf16 = jnp.float32, jnp.bfloat16
    dma = pltpu.SemaphoreType.DMA
    results = pl.pallas_call(
        exchange,
        name="exchange",
        out_shape=(
            pltpu.VMEM((48, 32, 2048), bf16),
            pltpu.VMEM((32, 128), f32),
            pltpu.VMEM((64, 2048), bf16),
            pltpu.VMEM((PAIRS, 8, 4, 32, 128), bf16),
            pltpu.VMEM((48, 32, 128), f32),
        ),
        in_specs=[hbm, hbm, hbm, vmem, vmem],
        out_specs=(vmem,) * 5,
        scratch_shapes=[
            pltpu.VMEM((48, 64, 1024), f32),
            pltpu.VMEM((PAIRS, 4, 8, 32, 128), bf16),
            pltpu.VMEM((PAIRS, 4, 8, 32, 128), bf16),
            pltpu.VMEM((2, 48, 1, 1024), f32),
            pltpu.VMEM((48, 1, 1024), f32),
            pltpu.VMEM((4, 8, 8, 128), bf16),
            pltpu.VMEM((4, 8, 8, 128), bf16),
            pltpu.VMEM((8, 4, 8, 128), bf16),
            pltpu.VMEM((2, 4, 4, 8, 128), bf16),
            pltpu.VMEM((2, 32, 2048), f32),
            dma((5,)),
            dma,
            dma((PAIRS,)),
            dma,
            dma((PAIRS,)),
            dma,
            dma,
            dma,
            dma,
            dma((3,)),
            dma((3,)),
            dma,
            dma,
            dma,
            dma,
        ],
        compiler_params=pltpu.CompilerParams(
            collective_id=0, has_side_effects=True, vmem_limit_bytes=49 * 2**20
        ),
    )(gate, up, jnp.swapaxes(down, 1, 2), weight.T, gain.reshape(1, 64))
    half = jax.ShapeDtypeStruct((16, 32, 2048), bf16)
    few = jax.ShapeDtypeStruct((16, 32), f32)
    gate, up, down, sg, su, sd, served = pl.pallas_call(
        hand_out,
        name="hand_out",
        out_shape=(half, half, half, few, few, few, jax.ShapeDtypeStruct((64, 2048), bf16)),
        in_specs=[vmem] * 5,
        out_specs=(hbm,) * 7,
        scratch_shapes=[
            pltpu.VMEM((4, 32, 2048), bf16),
            pltpu.VMEM((32, 128), f32),
            pltpu.VMEM((48, 32), f32),
            pltpu.VMEM((2, 32, 2048), f32),
            dma((8,)),
        ],
        compiler_params=pltpu.CompilerParams(vmem_limit_bytes=16 * 2**20),
    )(*(pltpu.with_memory_space_constraint(a, pltpu.VMEM) for a in results))
    return (
        jnp.swapaxes(gate, 1, 2),
        jnp.swapaxes(up, 1, 2),
        down,
        sg,
        su,
        sd,
        served.T,
    )


def solution(mesh):
    return jax.shard_map(
        body,
        mesh=mesh,
        in_specs=(
            P("bank", "zero", None),
            P("bank", "zero", None),
            P("bank", None, "zero"),
            P("zero", "bank"),
            P("zero"),
        ),
        out_specs=(
            P("bank", None, "zero"),
            P("bank", None, "zero"),
            P("bank", "zero", None),
            P("bank", "zero"),
            P("bank", "zero"),
            P("bank", "zero"),
            P(),
        ),
        check_vma=False,
    )
```

```python
import jax
import jax.numpy as jnp
from jax import lax
from jax.experimental import pallas as pl
from jax.experimental.pallas import tpu as pltpu
from jax.sharding import PartitionSpec as P

MESH = pl.DeviceIdType.MESH
CHUNKS = 12
OWN, SHARED = 16, 16
LAG = 4
AHEAD = 6
PAIRS = 24
POWER = 20
UP = 2.0**6.25


def turned(h, a, b):
    return a + h * (b - a), b + h * (a - b)


def left_half():
    return lax.broadcasted_iota(jnp.int32, (32, 128), 1) < 64


def decode_pair(recv, table, out, totals, wide, p, place):
    half = left_half()
    h = lax.rem(p, 2)
    f0 = table[2 * p]
    f1 = table[2 * p + 1]
    squares = [jnp.zeros((32, 128), jnp.float32)] * 2
    for t in range(16):
        z, x = t // 4, t % 4
        one, two = turned(h, z, x)
        left, right = 8 * z + x, 8 * z + 4 + x
        columns = slice(128 * t, 128 * t + 128)
        a = recv[p, 2 * one, two].astype(jnp.float32)
        b = recv[p, 2 * one + 1, two].astype(jnp.float32)
        for e, f, u in (
            (0, f0, jnp.where(half, a, pltpu.roll(b, 64, 1))),
            (1, f1, jnp.where(half, pltpu.roll(a, 64, 1), b)),
        ):
            g = jnp.where(
                half,
                jnp.broadcast_to(f[:, left : left + 1], (32, 128)),
                jnp.broadcast_to(f[:, right : right + 1], (32, 128)),
            )
            m = jnp.exp(jnp.log(jnp.abs(u)) * (1.0 / POWER))
            v = jnp.where(u < 0.0, -m, m) * g
            wide[e, :, columns] = v
            squares[e] = squares[e] + v * v
    lane = lax.broadcasted_iota(jnp.int32, (32, 128), 1)
    for e in range(2):
        total = jnp.sum(squares[e], axis=1, keepdims=True)
        totals[...] = jnp.where(lane == 2 * p + e, total, totals[...])
        r = lax.rsqrt(total)
        for t in range(16):
            columns = slice(128 * t, 128 * t + 128)
            out[2 * place + e, :, columns] = (wide[e, :, columns] * r).astype(jnp.bfloat16)


def exchange(
    gate, up, down, weight, gain,
    out, totals, router, recv, table,
    xin, send, relay, squares, sums, sums_send, sums_relay, sums_recv, parts, wide_rows,
    in_sem, send_sem, relay_sem, pass_sem, recv_sem,
    sums_send_sem, sums_relay_sem, sums_pass_sem, sums_recv_sem,
    parts_send_sem, parts_recv_sem, row_send_sem, row_recv_sem,
    mate_send_sem, mate_recv_sem,
):
    me = lax.axis_index("zero")
    bank = lax.axis_index("bank")
    mz, mx, mc = lax.div(me, 8), lax.rem(lax.div(me, 2), 4), lax.rem(me, 2)
    mate = 1 - mc

    def turn(place, i):
        return lax.rem(place + i, 4)

    def device(z, x, c):
        return z * 8 + x * 2 + c

    def put(src, dst, sent, arrived, z, x, c):
        pltpu.make_async_remote_copy(
            src_ref=src,
            dst_ref=dst,
            send_sem=sent,
            recv_sem=arrived,
            device_id={"zero": device(z, x, c)},
            device_id_type=MESH,
        ).start()

    def wait(ref, sem):
        pltpu.make_async_copy(ref, ref, sem).wait()

    barrier = pltpu.get_barrier_semaphore()

    def greet(**where):
        pl.semaphore_signal(
            barrier, inc=1, device_id=where, device_id_type=MESH
        )

    for i in (2, 1, 3):
        for c in range(2):
            greet(zero=device(turn(mz, i), mx, c))
            greet(zero=device(mz, turn(mx, i), c))
        greet(bank=turn(bank, i))
    greet(zero=device(mz, mx, mate))

    loads = [
        pltpu.make_async_copy(
            ref.at[pl.ds(k, count)], xin.at[pl.ds(16 * a + k, count)], in_sem.at[i]
        )
        for i, (a, ref, k, count) in enumerate(((0, gate, 0, 4), (0, gate, 4, 4), (0, gate, 8, 8), (1, up, 0, 16), (2, down, 0, 16)))
    ]
    for copy in loads[:2]:
        copy.start()

    part = (weight[...] * gain[...]).astype(jnp.bfloat16)
    row, spot = turned(mc, mz, mx)
    parts[mc, row, spot] = jnp.concatenate([part[0:8], part[8:16]], axis=1)

    def add_up(e, _):
        x = xin[e]
        squares[0, e] = jnp.sum(x * x, axis=0, keepdims=True)
        return 0

    def own_norm(e, _):
        x = xin[e]
        norm = jnp.sqrt(jnp.sum(x * x, axis=0, keepdims=True))
        sums[e] = norm.astype(jnp.bfloat16).astype(jnp.float32)
        return 0

    def chip_norm(e, _):
        norm = jnp.sqrt(squares[0, e] + squares[1, e])
        sums[e] = norm.astype(jnp.bfloat16).astype(jnp.float32)
        return 0

    def code(p):
        h = lax.rem(p, 2)
        for b in range(8):
            columns = slice(128 * b, 128 * b + 128)
            halves = []
            for e in range(2):
                s = sums[2 * p + e, :, columns]
                r = jnp.where(s > 0.0, UP / s, 0.0)
                halves.append(xin[2 * p + e, :, columns] * r)
            y = jnp.concatenate(halves, axis=0).T
            y2 = y * y
            y4 = y2 * y2
            y8 = y4 * y4
            y20 = y8 * y8 * y4
            u = jnp.where(y < 0.0, -y20, y20).astype(jnp.bfloat16)
            for q in range(4):
                z, x, d = b // 2, b % 2 * 2 + q // 2, q % 2
                first, second = turned(h, x, z)
                send[p, first, 2 * second + d] = u[32 * q : 32 * q + 32]

    def leave(p):
        h = lax.rem(p, 2)
        mine, other = turned(h, mx, mz)
        for i in (2, 1, 3):
            to = turn(mine, i)
            x, z = turned(h, to, other)
            put(send.at[p, to], relay.at[p, mine], send_sem, relay_sem.at[p], z, x, mc)
        relay[p, mine] = send[p, mine]

    four = pl.ds(0, 4)
    three = pl.ds(0, 3)

    def go_on(p):
        h = lax.rem(p, 2)
        wait(relay.at[p, three], relay_sem.at[p])
        mine, other = turned(h, mz, mx)
        slot = 2 * mine + mc
        put(relay.at[p, four, 2 * mine + mate], recv.at[p, slot], pass_sem, recv_sem.at[p], mz, mx, mate)
        for i in (2, 1, 3):
            to = turn(mine, i)
            z, x = turned(h, to, other)
            for d in range(2):
                put(relay.at[p, four, 2 * to + d], recv.at[p, slot], pass_sem, recv_sem.at[p], z, x, d)
        recv[p, slot] = relay[p, :, slot]

    def each(act, c):
        def go(p, _):
            act(p)
            return 0

        lax.fori_loop(2 * c, 2 * c + 2, go, 0)

    def code_and_leave(p):
        code(p)
        leave(p)

    loads[0].wait()
    lax.fori_loop(0, 4, own_norm, 0)
    each(code, 0)
    pl.semaphore_wait(barrier, 16)
    each(leave, 0)
    for copy in loads[2:]:
        copy.start()
    loads[1].wait()
    lax.fori_loop(4, 8, own_norm, 0)
    each(code_and_leave, 1)
    loads[2].wait()
    lax.fori_loop(8, OWN, own_norm, 0)
    each(code_and_leave, 2)
    each(code_and_leave, 3)

    for copy, low, high in zip(loads[3:], (16, 32), (32, 48)):
        copy.wait()
        lax.fori_loop(low, high, add_up, 0)
    rest = pl.ds(OWN, 48 - OWN)
    put(squares.at[0, rest], squares.at[1, rest], mate_send_sem, mate_recv_sem, mz, mx, mate)
    each(go_on, 0)
    wait(squares.at[1, rest], mate_recv_sem)
    lax.fori_loop(OWN, 48, chip_norm, 0)

    for b in range(8):
        columns = slice(128 * b, 128 * b + 128)
        s = jnp.concatenate(
            [
                sums[0:OWN, 0, columns],
                sums[pl.ds(OWN + SHARED * mc, SHARED), 0, columns],
            ],
            axis=0,
        )
        t = jnp.concatenate(
            [s] + [pltpu.roll(s, 128 - 8 * g, 1) for g in range(1, 4)], axis=0
        ).T
        for q in range(4):
            z, x, d = b // 2, b % 2 * 2 + q // 2, q % 2
            sums_send[x, 2 * z + d] = t[32 * q : 32 * q + 8].astype(jnp.bfloat16)
    for i in (1, 3, 2):
        x = turn(mx, i)
        put(sums_send.at[x], sums_relay.at[mx], sums_send_sem, sums_relay_sem, mz, x, mc)
        z_to, x_to = turned(mc, row, turn(spot, i))
        put(parts.at[mc, row, spot], parts.at[mc, row, spot], parts_send_sem.at[0], parts_recv_sem.at[0], z_to, x_to, mc)
    sums_relay[mx] = sums_send[mx]

    for c in range(4, AHEAD + 1):
        each(code_and_leave, c)
    each(go_on, 1)
    each(code_and_leave, AHEAD + 1)

    wait(sums_relay.at[three], sums_relay_sem)
    wait(parts.at[0, 0, three], parts_recv_sem.at[0])
    at_z = 2 * mz + mc
    for i in (1, 3, 2):
        z = turn(mz, i)
        for d in range(2):
            put(sums_relay.at[four, 2 * z + d], sums_recv.at[at_z], sums_pass_sem, sums_recv_sem, z, mx, d)
        z_to, x_to = turned(mc, turn(row, i), spot)
        put(parts.at[mc, row], parts.at[mc, row], parts_send_sem.at[1], parts_recv_sem.at[1], z_to, x_to, mc)
    put(sums_relay.at[four, 2 * mz + mate], sums_recv.at[at_z], sums_pass_sem, sums_recv_sem, mz, mx, mate)
    sums_recv[at_z] = sums_relay[:, at_z]

    for c in range(2, LAG):
        each(go_on, c)
        each(code_and_leave, AHEAD + c)

    wait(sums_recv.at[pl.ds(0, 7)], sums_recv_sem)
    wide = sums_recv[...].astype(jnp.float32).reshape(32, 8, 128)
    core = lax.rem(lax.div(lax.broadcasted_iota(jnp.int32, (128, 128), 1), 4), 2)
    for n in range(8):
        rows = jnp.concatenate([wide[:, n, :], jnp.zeros((96, 128), jnp.float32)], axis=0).T
        rows = rows * (1.0 / UP)
        low = jnp.where(core == 0, rows, pltpu.roll(rows, 4, 1))
        high = jnp.where(core == 1, rows, pltpu.roll(rows, 124, 1))
        for g in range(4):
            place = n + 8 * g
            own, chip = 32 * g, 32 * g + OWN
            table[0:OWN, place, :] = rows[own:chip]
            table[OWN : OWN + SHARED, place, :] = low[chip : chip + SHARED]
            table[OWN + SHARED : 48, place, :] = high[chip : chip + SHARED]
    totals[...] = jnp.zeros_like(totals)

    half = left_half()

    def decode(p):
        wait(recv.at[p, pl.ds(0, 7)], recv_sem.at[p])
        decode_pair(recv, table, out, totals, wide_rows, p, p)

    wait(parts.at[0, three], parts_recv_sem.at[1])
    put(parts.at[mc], parts.at[mc], parts_send_sem.at[2], parts_recv_sem.at[2], mz, mx, mate)

    mine = pl.ds(pl.multiple_of(16 * bank, 16), 16)

    def serve_rows():
        wait(parts.at[0], parts_recv_sem.at[2])
        low = half[0:8]
        for t in range(16):
            z, x = t // 4, t % 4
            a = parts[0, z, x].astype(jnp.float32)
            b = parts[1, x, z].astype(jnp.float32)
            block = jnp.concatenate(
                [
                    jnp.where(low, a, pltpu.roll(b, 64, 1)),
                    jnp.where(low, pltpu.roll(a, 64, 1), b),
                ],
                axis=0,
            )
            router[mine, 128 * t : 128 * t + 128] = block.astype(jnp.bfloat16)
        for i in range(1, 4):
            pltpu.make_async_remote_copy(
                src_ref=router.at[mine],
                dst_ref=router.at[mine],
                send_sem=row_send_sem,
                recv_sem=row_recv_sem,
                device_id={"bank": turn(bank, i)},
                device_id_type=MESH,
            ).start()

    def step(c, _):
        each(go_on, c)

        @pl.when(c < CHUNKS - AHEAD)
        def _():
            each(code_and_leave, c + AHEAD)

        each(decode, c - LAG)

        @pl.when(c == CHUNKS // 2)
        def _():
            serve_rows()

        return 0

    lax.fori_loop(LAG, CHUNKS, step, 0)
    for c in range(CHUNKS - LAG, CHUNKS - 1):
        each(decode, c)
    columns = pl.ds(0, 48)
    wait(router.at[columns], row_recv_sem)
    wait(router.at[columns], row_send_sem)
    wait(squares.at[1, rest], mate_send_sem)
    wait(parts.at[0, 0, three], parts_send_sem.at[0])
    wait(parts.at[0, three], parts_send_sem.at[1])
    wait(parts.at[0], parts_send_sem.at[2])
    wait(sums_send.at[three], sums_send_sem)
    wait(sums_recv.at[pl.ds(0, 7)], sums_pass_sem)
    every = pl.ds(0, PAIRS)
    wait(send.at[every, three], send_sem)
    for p in range(PAIRS - 2, PAIRS):
        wait(recv.at[p, pl.ds(0, 7)], recv_sem.at[p])
    wait(recv.at[every, pl.ds(0, 7)], pass_sem)


def hand_out(
    out, begun, router, recv, table,
    gate, up, down, sg, su, sd, served,
    last, totals, scale, wide_rows, sem,
):
    few = 4
    copies = []

    def copy(src, dst):
        copies.append(pltpu.make_async_copy(src, dst, sem.at[len(copies)]))
        copies[-1].start()

    for a, big in enumerate((gate, up, down)):
        count = 16 - few * (a == 2)
        copy(out.at[pl.ds(16 * a, count)], big.at[pl.ds(0, count)])
    copy(router, served)
    totals[...] = begun[...]

    def go(i, _):
        decode_pair(recv, table, last, totals, wide_rows, PAIRS - 2 + i, i)
        return 0

    lax.fori_loop(0, 2, go, 0)
    copy(last, down.at[pl.ds(16 - few, few)])
    across = jnp.concatenate([totals[...], jnp.zeros((96, 128), jnp.float32)], axis=0).T
    scale[...] = jnp.sqrt(across[0:48, 0:32])
    for a, small in enumerate((sg, su, sd)):
        copy(scale.at[pl.ds(16 * a, 16)], small)
    for c in copies:
        c.wait()


def body(gate, up, down, weight, gain):
    vmem = pl.BlockSpec(memory_space=pltpu.VMEM)
    hbm = pl.BlockSpec(memory_space=pltpu.HBM)
    f32, bf16 = jnp.float32, jnp.bfloat16
    dma = pltpu.SemaphoreType.DMA
    results = pl.pallas_call(
        exchange,
        name="exchange",
        out_shape=(
            pltpu.VMEM((48, 32, 2048), bf16),
            pltpu.VMEM((32, 128), f32),
            pltpu.VMEM((64, 2048), bf16),
            pltpu.VMEM((PAIRS, 8, 4, 32, 128), bf16),
            pltpu.VMEM((48, 32, 128), f32),
        ),
        in_specs=[hbm, hbm, hbm, vmem, vmem],
        out_specs=(vmem,) * 5,
        scratch_shapes=[
            pltpu.VMEM((48, 64, 1024), f32),
            pltpu.VMEM((PAIRS, 4, 8, 32, 128), bf16),
            pltpu.VMEM((PAIRS, 4, 8, 32, 128), bf16),
            pltpu.VMEM((2, 48, 1, 1024), f32),
            pltpu.VMEM((48, 1, 1024), f32),
            pltpu.VMEM((4, 8, 8, 128), bf16),
            pltpu.VMEM((4, 8, 8, 128), bf16),
            pltpu.VMEM((8, 4, 8, 128), bf16),
            pltpu.VMEM((2, 4, 4, 8, 128), bf16),
            pltpu.VMEM((2, 32, 2048), f32),
            dma((5,)),
            dma,
            dma((PAIRS,)),
            dma,
            dma((PAIRS,)),
            dma,
            dma,
            dma,
            dma,
            dma((3,)),
            dma((3,)),
            dma,
            dma,
            dma,
            dma,
        ],
        compiler_params=pltpu.CompilerParams(
            collective_id=0, has_side_effects=True, vmem_limit_bytes=49 * 2**20
        ),
    )(gate, up, jnp.swapaxes(down, 1, 2), weight.T, gain.reshape(1, 64))
    half = jax.ShapeDtypeStruct((16, 32, 2048), bf16)
    few = jax.ShapeDtypeStruct((16, 32), f32)
    gate, up, down, sg, su, sd, served = pl.pallas_call(
        hand_out,
        name="hand_out",
        out_shape=(half, half, half, few, few, few, jax.ShapeDtypeStruct((64, 2048), bf16)),
        in_specs=[vmem] * 5,
        out_specs=(hbm,) * 7,
        scratch_shapes=[
            pltpu.VMEM((4, 32, 2048), bf16),
            pltpu.VMEM((32, 128), f32),
            pltpu.VMEM((48, 32), f32),
            pltpu.VMEM((2, 32, 2048), f32),
            dma((8,)),
        ],
        compiler_params=pltpu.CompilerParams(vmem_limit_bytes=16 * 2**20),
    )(*(pltpu.with_memory_space_constraint(a, pltpu.VMEM) for a in results))
    return (
        jnp.swapaxes(gate, 1, 2),
        jnp.swapaxes(up, 1, 2),
        down,
        sg,
        su,
        sd,
        served.T,
    )


def solution(mesh):
    return jax.shard_map(
        body,
        mesh=mesh,
        in_specs=(
            P("bank", "zero", None),
            P("bank", "zero", None),
            P("bank", None, "zero"),
            P("zero", "bank"),
            P("zero"),
        ),
        out_specs=(
            P("bank", None, "zero"),
            P("bank", None, "zero"),
            P("bank", "zero", None),
            P("bank", "zero"),
            P("bank", "zero"),
            P("bank", "zero"),
            P(),
        ),
        check_vma=False,
    )
```
